256 devices in a mesh: dp: 32 (over z, y), mp: 8 (over x, core).
Axes of the slice: x: 4, y: 4, z: 8, core: 2. Of those that a mesh axis runs over, the one named last changes fastest.
Arguments:
- embedded: bfloat16 [128, 64, 4096], P('dp', None, 'mp'), may hold values from -6 to 6
- targets: int32 [128, 64], P('dp'), may hold values from 0 to 65535
- labels: int32 [128], P('dp'), may hold values from 0 to 21
- counts: int32 [32], replicated, may hold values from 0 to 4, as said below
- destinations: int32 [128], P('dp'), may hold values from 0 to 63, as said below
- gain_in: float32 [4096], replicated, may hold values from 0.1 to 1.9
- w_query: bfloat16 [4096, 2048], P(None, 'mp'), may hold values from -40 to 40
- w_key: bfloat16 [4096, 1024], P(None, 'mp'), may hold values from -0.09375 to 0.09375
- w_value: bfloat16 [4096, 1024], P(None, 'mp'), may hold values from -0.09375 to 0.09375
- w_out: bfloat16 [2048, 4096], P('mp'), may hold values from -0.5 to 0.5
- gain_out: float32 [4096], replicated, may hold values from 0.1 to 1.9
- w_vocab: bfloat16 [4096, 65536], P('mp', 'dp'), may hold values from -40 to 40
- prev_probs: float32 [22], replicated, may hold values from 0.03 to 0.2
- log_weights: float32 [22], replicated, may hold values from -200 to 21000
Outputs:
- token_loss: float32 [4096], P(('dp', 'mp'))
- new_weights: float32 [22], replicated
- probs: float32 [22], replicated
The draws below stay inside these ranges and needn't reach their ends.
Inputs may be any that keep to these rules, and one draw needn't show every extreme that they name: The counts sum to 64. `destinations`: each value from 0 to 63 is held by exactly one live slot; entries of slots that are not live are meaningless.
All inputs are finite; a program needn't handle non-finite values.
Results may differ from the reference program's by a relative error of at most 0.015.
The reference program's roundings to bfloat16 on the way count: a program that leaves them out, or rounds other values in their place, can miss the bound.
Values may be sent and summed in bfloat16 or wider, within the bound.
No kernel may reach another device: no remote copies, remote signals or barrier semaphores. Data moves between devices by JAX's collectives and lax.ppermute only.
A program may use at most 128 MiB of HBM per device.

```python
import math
import jax
import jax.numpy as jnp
from jax import lax

D = 4096
HEADS = 16
KV_HEADS = 8
HEAD_DIM = 128
VOCAB = 65536
DOMAINS = 22
SEQ_DEV = 2
SEQ_LEN = 64
SLOTS = 4
TOK_DEV = 128
N_DP = 32


def balance_plan(key):
    seeded = jax.random.fold_in(key, 91)
    key_order, key_shift, key_perm, key_fill = jax.random.split(seeded, 4)
    ordering = jax.random.permutation(key_order, N_DP)
    shifts = jax.random.randint(key_shift, (N_DP // 2,), 0, SEQ_DEV + 1)
    shifts = shifts.at[0].set(SEQ_DEV)
    paired = jnp.stack([SEQ_DEV + shifts, SEQ_DEV - shifts], axis=1).reshape(N_DP).astype(jnp.int32)
    counts = jnp.zeros((N_DP,), jnp.int32).at[ordering].set(paired)
    starts = jnp.cumsum(counts) - counts
    slot_ids = jnp.arange(N_DP * SLOTS, dtype=jnp.int32)
    device = slot_ids // SLOTS
    within = slot_ids % SLOTS
    is_live = within < counts[device]
    global_rank = jnp.minimum(starts[device] + within, N_DP * SEQ_DEV - 1)
    shuffled = jax.random.permutation(key_perm, N_DP * SEQ_DEV).astype(jnp.int32)
    filler = jax.random.randint(key_fill, (N_DP * SLOTS,), 0, N_DP * SEQ_DEV)
    destinations = jnp.where(is_live, shuffled[global_rank], filler).astype(jnp.int32)
    return (counts, destinations)


def draw_counts(key, part):
    return balance_plan(key)[0]


def draw_destinations(key, part):
    return balance_plan(key)[1]


def draw_w_query(key, part):
    key_base = jax.random.fold_in(jax.random.fold_in(key, 5), 0)
    entries = jax.random.normal(key_base, (D, HEADS * HEAD_DIM), jnp.float32) / math.sqrt(D)
    return jnp.clip(entries, -40.0, 40.0).astype(jnp.bfloat16)


def draw_w_vocab(key, part):
    key_base = jax.random.fold_in(jax.random.fold_in(key, 13), 0)
    entries = jax.random.normal(key_base, (D, VOCAB), jnp.float32) * (3.0 / math.sqrt(D))
    return jnp.clip(entries, -40.0, 40.0).astype(jnp.bfloat16)


def draw_log_weights(key, part):
    key_base = jax.random.fold_in(jax.random.fold_in(key, 17), 0)
    entries = jax.random.normal(key_base, (DOMAINS,), jnp.float32) * 20.0
    return entries


def set_ends(values, stream_key, smallest, top_value):
    longest = values.shape.index(max(values.shape))
    spots = []
    for shift in (0, 1):
        where = [jax.random.randint(jax.random.fold_in(stream_key, axis), (), 0, length) for axis, length in enumerate(values.shape)]
        where[longest] = (where[longest] + shift) % values.shape[longest]
        spots.append(tuple(where))
    return values.at[spots[0]].set(smallest).at[spots[1]].set(top_value)


def level_of(rng, shape, shards, low, top_value):
    level, own = 1.0, jax.random.fold_in(rng, 6)
    for axis_at, shards_of in shards:
        draws = jnp.exp(jax.random.uniform(jax.random.fold_in(own, axis_at), (shards_of,), jnp.float32, low / len(shards), top_value / len(shards)))
        level = level * jnp.repeat(draws, shape[axis_at] // shards_of).reshape([-1 if axis == axis_at else 1 for axis in range(len(shape))])
    return level


def gaussian(rng, dims, scale, reach, pieces=(), kind=jnp.bfloat16):
    values = scale * jax.random.normal(rng, dims, jnp.float32)
    if pieces:
        values = values * level_of(rng, dims, pieces, -0.22, 0.18)
    return jnp.clip(values, -reach, reach).astype(kind)


def setup_inputs(seed: int = 0) -> dict:
    splits = jax.random.split(jax.random.key(seed), 15)
    return {
        "embedded": gaussian(splits[0], (N_DP * SLOTS, SEQ_LEN, D), 1.0, 6.0, ((0, 32), (2, 8))),
        "targets": set_ends(jax.random.randint(splits[1], (N_DP * SLOTS, SEQ_LEN), 0, VOCAB), jax.random.fold_in(splits[1], 1), 0, VOCAB - 1).astype(jnp.int32),
        "labels": set_ends(jax.random.randint(splits[2], (N_DP * SLOTS,), 0, DOMAINS), jax.random.fold_in(splits[2], 1), 0, DOMAINS - 1).astype(jnp.int32),
        "counts": draw_counts(jax.random.fold_in(splits[14], 71), 0),
        "destinations": draw_destinations(jax.random.fold_in(splits[14], 71), 0),
        "gain_in": jnp.clip(1.0 + 0.18 * jax.random.normal(splits[5], (D,), jnp.float32), 0.1, 1.9),
        "w_query": draw_w_query(jax.random.fold_in(splits[14], 71), 0),
        "w_key": gaussian(splits[7], (D, KV_HEADS * HEAD_DIM), D ** -0.5, 0.09375, ((1, 8),)),
        "w_value": gaussian(splits[8], (D, KV_HEADS * HEAD_DIM), D ** -0.5, 0.09375, ((1, 8),)),
        "w_out": gaussian(splits[9], (HEADS * HEAD_DIM, D), (HEADS * HEAD_DIM // 16) ** -0.5, 0.5, ((0, 8),)),
        "gain_out": jnp.clip(1.0 + 0.18 * jax.random.normal(splits[10], (D,), jnp.float32), 0.1, 1.9),
        "w_vocab": draw_w_vocab(jax.random.fold_in(splits[14], 71), 0),
        "prev_probs": jnp.clip(jnp.exp(jax.random.uniform(splits[12], (DOMAINS,), jnp.float32, math.log(0.03), math.log(0.2))), 0.03, 0.2),
        "log_weights": draw_log_weights(jax.random.fold_in(splits[14], 71), 0),
    }


norm_eps = 1e-05
rope_base = 500000.0
memory_rate = 0.9
step_rate = 0.02
explore_mass = 0.005

def normalize(values, gain_vec):
    inv_rms = lax.rsqrt(lax.optimization_barrier(jnp.mean(values * values, axis=-1, keepdims=True)) + norm_eps)
    return values * inv_rms * gain_vec.astype(jnp.float32)

def rotate_halves(tensor):
    full_width = tensor.shape[-1]
    half_width = full_width // 2
    frequency = jnp.power(jnp.float32(rope_base), -jnp.arange(half_width, dtype=jnp.float32) * 2.0 / full_width)
    angles = jnp.arange(tensor.shape[1], dtype=jnp.float32)[:, None] * frequency[None, :]
    cosine = jnp.cos(angles)[None, :, None, :]
    sine_part = jnp.sin(angles)[None, :, None, :]
    first_half = tensor[..., :half_width]
    second = tensor[..., half_width:]
    return jnp.concatenate([first_half * cosine - second * sine_part, second * cosine + first_half * sine_part], axis=-1)

def reference(embedded, targets, labels, counts, destinations, gain_in, w_query, w_key, w_value, w_out, gain_out, w_vocab, prev_probs, log_weights):
    slot_ids = jnp.arange(N_DP * SLOTS, dtype=jnp.int32)
    is_live = slot_ids % SLOTS < counts[slot_ids // SLOTS]
    outputs = jnp.arange(N_DP * SEQ_DEV, dtype=jnp.int32)
    chosen = is_live[None, :] & (destinations[None, :] == outputs[:, None])
    source = lax.optimization_barrier(jnp.sum(jnp.where(chosen, slot_ids[None, :], 0), axis=1)).astype(jnp.int32)
    sequence_rows = embedded[source]
    seq_targets = targets[source]
    seq_labels = labels[source]
    groups = N_DP * SEQ_DEV
    tokens = groups * SEQ_LEN
    flat_rows = sequence_rows.reshape(tokens, D).astype(jnp.float32)
    normed = normalize(flat_rows, gain_in).astype(jnp.bfloat16)
    query_heads = jnp.dot(normed, w_query, preferred_element_type=jnp.float32).reshape(groups, SEQ_LEN, HEADS, HEAD_DIM)
    key_heads = jnp.dot(normed, w_key, preferred_element_type=jnp.float32).reshape(groups, SEQ_LEN, KV_HEADS, HEAD_DIM)
    value_heads = jnp.dot(normed, w_value, preferred_element_type=jnp.float32).astype(jnp.bfloat16).reshape(groups, SEQ_LEN, KV_HEADS, HEAD_DIM)
    query_heads = rotate_halves(query_heads).astype(jnp.bfloat16)
    key_heads = rotate_halves(key_heads).astype(jnp.bfloat16)
    group_size = HEADS // KV_HEADS
    key_heads = jnp.repeat(key_heads, group_size, axis=2)
    value_heads = jnp.repeat(value_heads, group_size, axis=2)
    scores = jnp.einsum('sqhe,skhe->shqk', query_heads.astype(jnp.float32), key_heads.astype(jnp.float32)) * HEAD_DIM ** (-0.5)
    causal = jnp.arange(SEQ_LEN)[:, None] >= jnp.arange(SEQ_LEN)[None, :]
    scores = jnp.where(causal[None, None], scores, -jnp.inf)
    weights = jax.nn.softmax(scores, axis=-1).astype(jnp.bfloat16)
    mixed_heads = jnp.einsum('shqk,skhe->sqhe', weights.astype(jnp.float32), value_heads.astype(jnp.float32))
    mixed_heads = mixed_heads.astype(jnp.bfloat16).reshape(tokens, HEADS * HEAD_DIM)
    update = jnp.dot(mixed_heads, w_out, preferred_element_type=jnp.float32)
    hidden = flat_rows + update
    final_rows = normalize(hidden, gain_out).astype(jnp.bfloat16)
    token_targets = seq_targets.reshape(tokens)
    block_size = TOK_DEV
    block_count = tokens // block_size

    def block_loss(inputs):
        row_block, goal_ids = inputs
        logits = jnp.dot(row_block, w_vocab, preferred_element_type=jnp.float32)
        row_top = lax.optimization_barrier(jnp.max(logits, axis=1))
        spread = lax.optimization_barrier(jnp.sum(jnp.exp(logits - row_top[:, None]), axis=1))
        picked = jnp.take_along_axis(logits, goal_ids[:, None].astype(jnp.int32), axis=1)[:, 0]
        return row_top + jnp.log(spread) - picked
    losses = lax.map(block_loss, (final_rows.reshape(block_count, block_size, D), token_targets.reshape(block_count, block_size)))
    losses = losses.reshape(tokens)
    token_labels = jnp.repeat(seq_labels, SEQ_LEN)
    member = (token_labels[:, None] == jnp.arange(DOMAINS, dtype=jnp.int32)[None, :]).astype(jnp.float32)
    loss_sums = lax.optimization_barrier(jnp.sum(member * losses[:, None], axis=0))
    token_tally = lax.optimization_barrier(jnp.sum(member, axis=0))
    reward = loss_sums / jnp.maximum(token_tally, 1.0) / prev_probs
    new_weights = memory_rate * log_weights + (1.0 - memory_rate) * reward
    probs = (1.0 - DOMAINS * explore_mass) * jax.nn.softmax(step_rate * new_weights) + explore_mass
    return (losses, new_weights, probs)
```

```python
import functools

import jax
import jax.numpy as jnp
import numpy as np
from jax import lax
from jax.experimental import pallas as pl
from jax.experimental.pallas import tpu as pltpu
from jax.sharding import Mesh
from jax.sharding import PartitionSpec as P

HEAD_DIM = 128
DOMAINS = 22
SEQ_LEN = 64
DP = ("z", "y")
MP = ("x", "c")
ALL = ("z", "y", "x", "c")
NZ, NY, NX, NC = 8, 4, 4, 2

norm_eps = 1e-05
rope_base = 500000.0
memory_rate = 0.9
step_rate = 0.02
explore_mass = 0.005


bf16 = jnp.bfloat16
f32 = jnp.float32
i32 = jnp.int32


def shift(array, axis, by):
    n = {"z": NZ, "y": NY, "x": NX, "c": NC}[axis]
    return lax.ppermute(array, axis, [(i, (i + by) % n) for i in range(n)])


def call(kernel, out_shape, args, scalars=None, scratch=(), name=None, flops=0, vmem=None):
    spec = pl.BlockSpec(memory_space=pltpu.VMEM)
    many = isinstance(out_shape, (list, tuple))
    params = {} if vmem is None else {"vmem_limit_bytes": vmem}
    return pl.pallas_call(
        kernel,
        out_shape=out_shape,
        in_specs=([pl.BlockSpec(memory_space=pltpu.SMEM)] if scalars is not None else [])
        + [spec] * len(args),
        out_specs=[spec] * len(out_shape) if many else spec,
        scratch_shapes=scratch,
        name=name,
        compiler_params=pltpu.CompilerParams(**params),
        cost_estimate=pl.CostEstimate(flops=flops, bytes_accessed=0, transcendentals=0)
        if flops
        else None,
    )(*(() if scalars is None else (scalars,)), *args)


def sds(shape, dtype):
    return jax.ShapeDtypeStruct(shape, dtype)


def select_kernel(row_ref, got_ref, out_ref):
    for g in range(64):
        out_ref[g] = got_ref[row_ref[g]]


def rope_tables():
    half = HEAD_DIM // 2
    frequency = np.power(rope_base, -np.arange(half) * 2.0 / HEAD_DIM)
    angle = np.arange(SEQ_LEN)[:, None] * frequency[None, :]
    cosine = np.concatenate([np.cos(angle), np.cos(angle)], axis=1)
    sine = np.concatenate([-np.sin(angle), np.sin(angle)], axis=1)
    both = [np.concatenate([t, t], axis=0).astype(np.float32) for t in (cosine, sine)]
    return both


def attention_kernel(
    at_ref, b0, b1, b2, b3, o0, o1, o2, o3, gain, wq, wk, wv, wo, cos, sin,
    keep_ref, send_ref, resid_ref, mixed_ref,
):
    x, c = at_ref[0], at_ref[1]
    m = x * 2 + c
    blocks = [b0, b1, b2, b3, o0, o1, o2, o3]

    def feature_block(k):
        return lax.rem(x + (4 - k % 4), 4) * 2 + (c if k < 4 else 1 - c)

    def piece(ref, col):
        return jnp.concatenate([ref[r * 4 + col] for r in range(8)], axis=0).astype(f32)

    squares = jnp.zeros((128, 128), f32)
    for ref in blocks:
        for col in range(4):
            v = piece(ref, col)
            squares = squares + v * v
    inv_rms = lax.rsqrt(jnp.sum(squares, axis=1, keepdims=True) * (1.0 / 4096.0) + norm_eps)

    query = jnp.zeros((128, 256), f32)
    key = jnp.zeros((128, 128), f32)
    value = jnp.zeros((128, 128), f32)
    for k, ref in enumerate(blocks):
        fb = feature_block(k)
        g = gain[fb]
        normed = jnp.concatenate(
            [
                (piece(ref, col) * inv_rms * g[:, col * 128 : col * 128 + 128]).astype(bf16)
                for col in range(4)
            ],
            axis=1,
        )
        rows = pl.ds(pl.multiple_of(fb * 512, 512), 512)
        query = query + jnp.dot(normed, wq[rows, :], preferred_element_type=f32)
        key = key + jnp.dot(normed, wk[rows, :], preferred_element_type=f32)
        value = value + jnp.dot(normed, wv[rows, :], preferred_element_type=f32)

    def in_order(t):
        return jnp.concatenate(
            [t[r * 16 + s * 8 : r * 16 + s * 8 + 8] for s in range(2) for r in range(8)], axis=0
        )

    cosine, sine = cos[...], sin[...]

    def rotated(t):
        return (t * cosine + pltpu.roll(t, 64, axis=1) * sine).astype(bf16)

    query, key, value = in_order(query), rotated(in_order(key)), in_order(value).astype(bf16)
    row = lax.broadcasted_iota(i32, (128, 128), 0)
    column = lax.broadcasted_iota(i32, (128, 128), 1)
    seen = (row // SEQ_LEN == column // SEQ_LEN) & (column <= row)
    for h in range(2):
        q = rotated(query[:, h * 128 : h * 128 + 128])
        scores = lax.dot_general(q, key, (((1,), (1,)), ((), ())), preferred_element_type=f32)
        scores = jnp.where(seen, scores * HEAD_DIM ** (-0.5), -jnp.inf)
        top = jnp.max(scores, axis=1, keepdims=True)
        e = jnp.exp(scores - top)
        weights = (e / jnp.sum(e, axis=1, keepdims=True)).astype(bf16)
        mixed = jnp.dot(weights, value, preferred_element_type=f32).astype(bf16)
        mixed_ref[:, :, h * 128 : h * 128 + 128] = mixed.reshape(8, 16, 128)
    left = jnp.concatenate(
        [mixed_ref[t * 2 + c] for t in range(4)] + [mixed_ref[t * 2 + 1 - c] for t in range(4)],
        axis=0,
    )
    for fb in range(8):
        part = jnp.dot(left, wo[:, fb * 512 : fb * 512 + 512], preferred_element_type=f32)
        part = part.astype(bf16).reshape(8, 16, 512)
        keep_ref[:, fb] = part[:4]
        send_ref[:, fb] = part[4:]

    first = m < 4
    r0 = lax.rem(m, 4) * 2
    for k, ref in enumerate(blocks):
        fb = feature_block(k)
        rows = []
        for r in range(2):
            cols = []
            for col in range(4):
                v = ref[(r0 + r) * 4 + col].astype(f32)
                cols.append(jnp.where(first, v[:8], v[8:]))
            rows.append(jnp.concatenate(cols, axis=1))
        resid_ref[fb] = jnp.concatenate(rows, axis=0).astype(bf16)


def pair_kernel(at_ref, keep_ref, got_ref, own_ref, s1_ref, s2_ref, s3_ref):
    x = at_ref[0]
    for s, ref in enumerate((own_ref, s1_ref, s2_ref, s3_ref)):
        to = lax.rem(x + s, 4)
        ref[...] = (keep_ref[to].astype(f32) + got_ref[to].astype(f32)).astype(ref.dtype)


def final_kernel(at_ref, resid, own, r1, r2, r3, gain, fa_ref, fb_ref, hidden_ref):
    x, c = at_ref[0], at_ref[1]
    squares = jnp.zeros((16, 512), f32)
    for k in range(8):
        h = resid[k].astype(f32) + (
            own[k] + r1[k].astype(f32) + r2[k].astype(f32) + r3[k].astype(f32)
        )
        hidden_ref[k] = h
        squares = squares + h * h
    inv_rms = lax.rsqrt(jnp.sum(squares, axis=1, keepdims=True) * (1.0 / 4096.0) + norm_eps)
    for s in range(4):
        base = lax.rem(x + (4 - s), 4) * 2
        for out, core in ((fa_ref, c), (fb_ref, 1 - c)):
            out[s] = (hidden_ref[base + core] * inv_rms * gain[base + core]).astype(bf16)


def place(z, y, dz, dy):
    return lax.rem(z + (8 - dz), 8) * 4 + lax.rem(y + (4 - dy), 4)


def first_kernel(at_ref, *refs):
    g = refs[:8]
    w = refs[8:16]
    out_ref, rows_ref = refs[16:]

    @pl.when(pl.program_id(0) == 0)
    def _():
        z, y = at_ref[2], at_ref[3]
        for dz in range(8):
            for dy in range(4):
                to = place(z, y, dz, dy)
                for k in range(4):
                    rows_ref[k, to] = g[dz][dy, k]

    total = None
    for k in range(4):
        rows = rows_ref[k].reshape(512, 512)
        for half in range(2):
            part = jnp.dot(
                rows[:, half * 256 : half * 256 + 256], w[k * 2 + half][...],
                preferred_element_type=f32,
            )
            total = part if total is None else total + part
    out_ref[...] = total


def second_kernel(at_ref, *refs):
    g = refs[:4]
    w = refs[4:12]
    part_ref, goal_ref, out_ref, rows_ref, top_ref, sum_ref, pick_ref = refs[12:]
    step = pl.program_id(0)

    @pl.when(step == 0)
    def _():
        z, y = at_ref[2], at_ref[3]
        for dz in range(8):
            for dy in range(4):
                to = place(z, y, dz, dy)
                for k in range(4):
                    rows_ref[k, to] = g[dy][dz, k]
        top_ref[...] = jnp.full((512, 1), -jnp.inf, f32)
        sum_ref[...] = jnp.zeros((512, 1), f32)
        pick_ref[...] = jnp.zeros((512, 1), f32)

    total = part_ref[...]
    for k in range(4):
        rows = rows_ref[k].reshape(512, 512)
        for half in range(2):
            total = total + jnp.dot(
                rows[:, half * 256 : half * 256 + 256], w[k * 2 + half][...],
                preferred_element_type=f32,
            )
    width = total.shape[1]
    column = lax.broadcasted_iota(i32, total.shape, 1) + step * width
    old = top_ref[...]
    top = jnp.maximum(old, jnp.max(total, axis=1, keepdims=True))
    sum_ref[...] = sum_ref[...] * jnp.exp(old - top) + jnp.sum(
        jnp.exp(total - top), axis=1, keepdims=True
    )
    top_ref[...] = top
    pick_ref[...] += jnp.sum(
        jnp.where(column == goal_ref[...], total, 0.0), axis=1, keepdims=True
    )

    @pl.when(step == pl.num_programs(0) - 1)
    def _():
        eye = lax.broadcasted_iota(i32, (128, 128), 0) == lax.broadcasted_iota(
            i32, (128, 128), 1
        )
        lines = []
        for column_values in (top_ref[...] + jnp.log(sum_ref[...]), pick_ref[...]):
            for q in range(4):
                lines.append(
                    jnp.sum(
                        jnp.where(eye, column_values[q * 128 : q * 128 + 128], 0.0),
                        axis=0,
                        keepdims=True,
                    )
                )
        out_ref[...] = jnp.broadcast_to(jnp.concatenate(lines, axis=0)[None], (32, 8, 128))


def logits_call(kernel, rows, weights, extra, extra_specs, out_shape, out_spec, scratch, at, name):
    blocks = 4
    width = 2048 // blocks
    whole = lambda a: pl.BlockSpec(a.shape, functools.partial(lambda n, j, at: (0,) * n, a.ndim))
    half = lambda h: pl.BlockSpec((256, width), lambda j, at: (h, j))
    return pl.pallas_call(
        kernel,
        out_shape=out_shape,
        grid_spec=pltpu.PrefetchScalarGridSpec(
            num_scalar_prefetch=1,
            grid=(blocks,),
            in_specs=[whole(a) for a in rows] + [half(h) for _, h in weights] + extra_specs(width),
            out_specs=out_spec(width),
            scratch_shapes=scratch,
        ),
        name=name,
        cost_estimate=pl.CostEstimate(
            flops=2 * 512 * 2048 * 2048, bytes_accessed=12 << 20, transcendentals=0
        ),
    )(at, *rows, *(w for w, _ in weights), *extra)


def merge_kernel(got_ref, label_ref, loss_ref, sums_ref):
    lse = [got_ref[k][:4] for k in range(32)]
    top = functools.reduce(jnp.maximum, lse)
    total = functools.reduce(lambda a, b: a + b, [jnp.exp(v - top) for v in lse])
    picked = functools.reduce(lambda a, b: a + b, [got_ref[k][4:] for k in range(32)])
    loss = top + jnp.log(total) - picked
    loss_ref[...] = loss
    domain = lax.broadcasted_iota(i32, (128, 128), 0)
    by_domain = jnp.zeros((128, 128), f32)
    for q in range(4):
        same = domain == label_ref[q : q + 1, :]
        by_domain = by_domain + jnp.where(same, loss[q : q + 1, :], 0.0)
    column = jnp.sum(by_domain, axis=1, keepdims=True)
    eye = domain == lax.broadcasted_iota(i32, (128, 128), 1)
    line = jnp.sum(jnp.where(eye, column, 0.0), axis=0, keepdims=True)
    sums_ref[...] = jnp.broadcast_to(line, (8, 128))


def output_kernel(at_ref, s0, s1, s2, s3, tally, prev, old, new_ref, probs_ref, all_ref):
    x = at_ref[0]
    for s, ref in enumerate((s0, s1, s2, s3)):
        all_ref[lax.rem(x + (4 - s), 4)] = ref[...]
    sums = ((all_ref[0] + all_ref[1]) + (all_ref[2] + all_ref[3]))[0:1]
    reward = sums / jnp.maximum(tally[...], 1.0) / prev[...]
    new = memory_rate * old[...] + (1.0 - memory_rate) * reward
    real = lax.broadcasted_iota(i32, (1, 128), 1) < DOMAINS
    scaled = jnp.where(real, step_rate * new, -jnp.inf)
    e = jnp.exp(scaled - jnp.max(scaled, axis=1, keepdims=True))
    soft = e / jnp.sum(e, axis=1, keepdims=True)
    new_ref[...] = new
    probs_ref[...] = (1.0 - DOMAINS * explore_mass) * soft + explore_mass


def local(
    embedded, targets, labels, counts, destinations, gain_in, w_query, w_key, w_value, w_out,
    gain_out, w_vocab, prev_probs, log_weights,
):
    z, y, x, c = (lax.axis_index(a) for a in ALL)
    d, m = z * NY + y, x * NC + c
    at = jnp.stack([x, c, z, y]).astype(i32)

    def spread(rows):
        return [rows] + [shift(rows, "x", s) for s in (1, 3, 2)]

    def in_sequence(parts):
        return [parts[0], parts[1], parts[3], parts[2]]

    w_first = in_sequence(spread(w_vocab[:256]))

    tiles = embedded.reshape(4, 8, 8, 4, 128).transpose(1, 3, 0, 2, 4).reshape(32, 4, 8, 128)
    ids = jnp.concatenate([targets // 256, targets % 256], axis=1)
    info = jnp.pad(jnp.concatenate([labels, destinations])[None, :], ((0, 3), (0, 120)))
    meta = jnp.concatenate([ids, info], axis=0).astype(bf16)
    packed = jnp.concatenate([tiles, jnp.broadcast_to(meta, (32, 1, 8, 128))], axis=1)
    got = lax.all_to_all(packed, DP, 0, 0, tiled=True)

    meta = got[:, 4]
    label_of = meta[:, 4, 0:4].reshape(128).astype(i32)
    goes_to = meta[:, 4, 4:8].reshape(128).astype(i32)
    slot = jnp.arange(128, dtype=i32)
    live = slot % 4 < jnp.repeat(counts, 4)
    chosen = live[None, :] & (goes_to[None, :] == jnp.arange(64, dtype=i32)[:, None])
    source_row = jnp.sum(jnp.where(chosen, (slot // 4) * 5 + slot % 4, 0), axis=1)
    picked = call(
        select_kernel, sds((64, 8, 128), bf16), (got.reshape(160, 8, 128),), source_row,
        name="select",
    )
    block = lax.all_to_all(picked.reshape(32, 16, 128), DP, 0, 0, tiled=True)

    blocks = [block] + [shift(block, "x", s) for s in (1, 2, 3)]
    others = [shift(b, "c", 1) for b in blocks]

    cosine, sine = rope_tables()
    keep, send, resid = call(
        attention_kernel,
        [sds((4, 8, 16, 512), bf16), sds((4, 8, 16, 512), bf16), sds((8, 16, 512), bf16)],
        (
            *blocks, *others, gain_in.reshape(8, 1, 512), w_query, w_key, w_value, w_out,
            jnp.asarray(cosine), jnp.asarray(sine),
        ),
        at,
        scratch=[pltpu.VMEM((8, 16, 256), bf16)],
        name="attention",
        flops=1 << 30,
    )
    other = shift(send, "c", 1)
    part = sds((8, 16, 512), bf16)
    own, *sends = call(
        pair_kernel, [sds((8, 16, 512), f32), part, part, part], (keep, other), at, name="pair"
    )
    sums = [shift(t, "x", s + 1) for s, t in enumerate(sends)]
    fa, fb = call(
        final_kernel, [sds((4, 16, 512), bf16)] * 2,
        (resid, own, *sums, gain_out.reshape(8, 1, 512)), at,
        scratch=[pltpu.VMEM((8, 16, 512), f32)], name="final",
    )

    held, _ = lax.optimization_barrier((w_vocab[256:], sums))
    w_second = in_sequence(spread(held))
    w_other = shift(w_vocab, "c", 1)
    w_first_other = [shift(t, "c", 1) for t in w_first[1:]]
    w_second_other = [shift(t, "c", 1) for t in w_second[1:]]

    group = jnp.stack([fa] + [shift(fa, "y", s) for s in (1, 2, 3)])
    up, down = [group], [group]
    for _ in range(3):
        up.append(shift(up[-1], "z", 1))
        down.append(shift(down[-1], "z", NZ - 1))
    up.append(shift(up[-1], "z", 1))
    rows_a = [*up, down[3], down[2], down[1]]
    up, down = [fb], [fb]
    for _ in range(3):
        up.append(shift(up[-1], "z", 1))
        down.append(shift(down[-1], "z", NZ - 1))
    up.append(shift(up[-1], "z", 1))
    column = jnp.stack([*up, down[3], down[2], down[1]])
    rows_b = [column] + [shift(column, "y", s) for s in (1, 2, 3)]

    chosen_slots = chosen.astype(bf16)
    seq_ids = jnp.dot(
        chosen_slots, meta[:, :4].reshape(128, 128), preferred_element_type=f32
    ).astype(i32)
    seq_goals = seq_ids[:, :64] * 256 + seq_ids[:, 64:]
    seq_labels = jnp.sum(jnp.where(chosen, label_of[None, :], 0), axis=1)
    mine = lax.dynamic_slice(
        seq_goals.reshape(32, 2, 4, 16), (0, m // 4, m % 4, 0), (32, 1, 1, 16)
    ).reshape(512)
    kinds = lax.dynamic_slice(seq_labels.reshape(32, 2), (0, m // 4), (32, 1))
    kinds = jnp.broadcast_to(kinds, (32, 16)).reshape(4, 128)
    goals = (mine - d * 2048).reshape(512, 1)
    domain = jnp.arange(128, dtype=i32)
    tally = SEQ_LEN * jnp.sum(
        (live[:, None] & (label_of[:, None] == domain[None, :])).astype(f32), axis=0
    )

    weights_a = [(w_vocab, 0), (w_vocab, 1)]
    weights_b = [(w_other, 0), (w_other, 1)]
    for s in range(3):
        weights_a += [(w_first[s + 1], 0), (w_second[s + 1], 0)]
        weights_b += [(w_first_other[s], 0), (w_second_other[s], 0)]
    partial = logits_call(
        first_kernel, rows_a, weights_a, (), lambda w: [], sds((512, 2048), f32),
        lambda w: pl.BlockSpec((512, w), lambda j, at: (0, j)),
        [pltpu.VMEM((4, 32, 16, 512), bf16)], at, "logits_first",
    )
    pieces = logits_call(
        second_kernel, rows_b, weights_b, (partial, goals),
        lambda w: [
            pl.BlockSpec((512, w), lambda j, at: (0, j)),
            pl.BlockSpec((512, 1), lambda j, at: (0, 0)),
        ],
        sds((32, 8, 128), f32), lambda w: pl.BlockSpec((32, 8, 128), lambda j, at: (0, 0, 0)),
        [pltpu.VMEM((4, 32, 16, 512), bf16)] + [pltpu.VMEM((512, 1), f32)] * 3, at,
        "logits_second",
    )
    merged = lax.all_to_all(pieces, DP, 0, 0, tiled=True)
    losses, sums_here = call(
        merge_kernel, [sds((4, 128), f32), sds((8, 128), f32)], (merged, kinds), name="merge"
    )
    own_loss = lax.dynamic_slice_in_dim(losses.reshape(512), d * 16, 16, 0)
    chip_sums = sums_here + shift(sums_here, "c", 1)
    all_sums = [chip_sums] + [shift(chip_sums, "x", s) for s in (1, 2, 3)]
    line = lambda v, fill: jnp.pad(v, (0, 128 - DOMAINS), constant_values=fill).reshape(1, 128)
    new_weights, probs = call(
        output_kernel, [sds((1, 128), f32)] * 2,
        (*all_sums, tally.reshape(1, 128), line(prev_probs, 1.0), line(log_weights, 0.0)), at,
        scratch=[pltpu.VMEM((4, 8, 128), f32)], name="output",
    )
    return own_loss, new_weights[0, :DOMAINS], probs[0, :DOMAINS]


def solution(mesh):
    torus = Mesh(mesh.devices.reshape(NZ, NY, NX, NC), ALL)
    in_specs = (
        P(DP, None, MP), P(DP, None), P(DP), P(), P(DP), P(), P(None, MP), P(None, MP),
        P(None, MP), P(MP, None), P(), P(MP, DP), P(), P(),
    )
    return jax.shard_map(
        local, mesh=torus, in_specs=in_specs, out_specs=(P(ALL), P(), P()), check_vma=False
    )
```

```python
import functools

import jax
import jax.numpy as jnp
import numpy as np
from jax import lax
from jax.experimental import pallas as pl
from jax.experimental.pallas import tpu as pltpu
from jax.sharding import Mesh
from jax.sharding import PartitionSpec as P


HEAD_DIM = 128
DOMAINS = 22
SEQ_LEN = 64
DP = ("z", "y")
MP = ("x", "c")
ALL = ("z", "y", "x", "c")
NZ, NY, NX, NC = 8, 4, 4, 2

norm_eps = 1e-05
rope_base = 500000.0
memory_rate = 0.9
step_rate = 0.02
explore_mass = 0.005


bf16 = jnp.bfloat16
f32 = jnp.float32
i32 = jnp.int32


def shift(array, axis, by):
    n = {"z": NZ, "y": NY, "x": NX, "c": NC}[axis]
    return lax.ppermute(array, axis, [(i, (i + by) % n) for i in range(n)])


def call(kernel, out_shape, args, scalars=None, scratch=(), flops=0, vmem=None):
    spec = pl.BlockSpec(memory_space=pltpu.VMEM)
    many = isinstance(out_shape, (list, tuple))
    params = {} if vmem is None else {"vmem_limit_bytes": vmem}
    return pl.pallas_call(
        kernel,
        out_shape=out_shape,
        in_specs=([pl.BlockSpec(memory_space=pltpu.SMEM)] if scalars is not None else [])
        + [spec] * len(args),
        out_specs=[spec] * len(out_shape) if many else spec,
        scratch_shapes=scratch,
        compiler_params=pltpu.CompilerParams(**params),
        cost_estimate=pl.CostEstimate(flops=flops, bytes_accessed=0, transcendentals=0)
        if flops
        else None,
    )(*(() if scalars is None else (scalars,)), *args)


def sds(shape, dtype):
    return jax.ShapeDtypeStruct(shape, dtype)


def pack_kernel(embedded, targets, labels, destinations, out_ref, meta_ref):
    ids = targets[...]
    meta_ref[...] = jnp.zeros((8, 128), f32)
    meta_ref[0:4, 0:64] = (ids // 256).astype(f32)
    meta_ref[0:4, 64:128] = (ids % 256).astype(f32)
    meta_ref[4:5, 0:4] = labels[...].astype(f32)
    meta_ref[5:6, 0:4] = destinations[...].astype(f32)
    meta = meta_ref[...].astype(bf16)
    for r in range(8):
        for col in range(4):
            for s in range(4):
                out_ref[r * 4 + col, s] = embedded[
                    s, r * 8 : r * 8 + 8, col * 128 : col * 128 + 128
                ]
            out_ref[r * 4 + col, 4] = meta


def select_kernel(row_ref, got_ref, out_ref):
    for g in range(64):
        out_ref[g] = got_ref[row_ref[g]]


def rope_tables():
    half = HEAD_DIM // 2
    frequency = np.power(rope_base, -np.arange(half) * 2.0 / HEAD_DIM)
    angle = np.arange(SEQ_LEN)[:, None] * frequency[None, :]
    cosine = np.concatenate([np.cos(angle), np.cos(angle)], axis=1)
    sine = np.concatenate([-np.sin(angle), np.sin(angle)], axis=1)
    both = [np.concatenate([t, t], axis=0).astype(np.float32) for t in (cosine, sine)]
    return both


def attention_kernel(
    at_ref, same, other, gain, wq, wk, wv, wo, cos, sin, keep_ref, send_ref, resid_ref, mixed_ref
):
    x, c = at_ref[0], at_ref[1]
    m = x * 2 + c
    blocks = [same.at[t] for t in range(4)] + [other.at[t] for t in range(4)]

    def feature_block(k):
        return (k % 4) * 2 + (c if k < 4 else 1 - c)

    def piece(ref, col):
        return jnp.concatenate([ref[r * 4 + col] for r in range(8)], axis=0).astype(f32)

    squares = jnp.zeros((128, 128), f32)
    for ref in blocks:
        for col in range(4):
            v = piece(ref, col)
            squares = squares + v * v
    inv_rms = lax.rsqrt(jnp.sum(squares, axis=1, keepdims=True) * (1.0 / 4096.0) + norm_eps)

    query = jnp.zeros((128, 256), f32)
    key = jnp.zeros((128, 128), f32)
    value = jnp.zeros((128, 128), f32)
    for k, ref in enumerate(blocks):
        fb = feature_block(k)
        g = gain[fb]
        normed = jnp.concatenate(
            [
                (piece(ref, col) * inv_rms * g[:, col * 128 : col * 128 + 128]).astype(bf16)
                for col in range(4)
            ],
            axis=1,
        )
        rows = pl.ds(pl.multiple_of(fb * 512, 512), 512)
        query = query + jnp.dot(normed, wq[rows, :], preferred_element_type=f32)
        key = key + jnp.dot(normed, wk[rows, :], preferred_element_type=f32)
        value = value + jnp.dot(normed, wv[rows, :], preferred_element_type=f32)

    def in_order(t):
        return jnp.concatenate(
            [t[r * 16 + s * 8 : r * 16 + s * 8 + 8] for s in range(2) for r in range(8)], axis=0
        )

    cosine, sine = cos[...], sin[...]

    def rotated(t):
        return (t * cosine + pltpu.roll(t, 64, axis=1) * sine).astype(bf16)

    query, key, value = in_order(query), rotated(in_order(key)), in_order(value).astype(bf16)
    row = lax.broadcasted_iota(i32, (128, 128), 0)
    column = lax.broadcasted_iota(i32, (128, 128), 1)
    seen = (row // SEQ_LEN == column // SEQ_LEN) & (column <= row)
    for h in range(2):
        q = rotated(query[:, h * 128 : h * 128 + 128])
        scores = lax.dot_general(q, key, (((1,), (1,)), ((), ())), preferred_element_type=f32)
        scores = jnp.where(seen, scores * HEAD_DIM ** (-0.5), -jnp.inf)
        top = jnp.max(scores, axis=1, keepdims=True)
        e = jnp.exp(scores - top)
        weights = (e / jnp.sum(e, axis=1, keepdims=True)).astype(bf16)
        mixed = jnp.dot(weights, value, preferred_element_type=f32).astype(bf16)
        mixed_ref[:, :, h * 128 : h * 128 + 128] = mixed.reshape(8, 16, 128)
    left = jnp.concatenate(
        [mixed_ref[t * 2 + c] for t in range(4)] + [mixed_ref[t * 2 + 1 - c] for t in range(4)],
        axis=0,
    )
    for fb in range(8):
        part = jnp.dot(left, wo[:, fb * 512 : fb * 512 + 512], preferred_element_type=f32)
        part = part.astype(bf16).reshape(8, 16, 512)
        keep_ref[:, fb] = part[:4]
        send_ref[:, fb] = part[4:]

    first = m < 4
    r0 = lax.rem(m, 4) * 2
    for k, ref in enumerate(blocks):
        fb = feature_block(k)
        rows = []
        for r in range(2):
            cols = []
            for col in range(4):
                v = ref[(r0 + r) * 4 + col].astype(f32)
                cols.append(jnp.where(first, v[:8], v[8:]))
            rows.append(jnp.concatenate(cols, axis=1))
        resid_ref[fb] = jnp.concatenate(rows, axis=0).astype(bf16)


def pair_kernel(keep_ref, got_ref, out_ref):
    out_ref[...] = (keep_ref[...].astype(f32) + got_ref[...].astype(f32)).astype(bf16)


def final_kernel(at_ref, resid, sums, gain, fa_ref, fb_ref, hidden_ref):
    x, c = at_ref[0], at_ref[1]
    squares = jnp.zeros((16, 512), f32)
    for k in range(8):
        h = resid[k].astype(f32) + (
            (sums[0, k].astype(f32) + sums[1, k].astype(f32))
            + (sums[2, k].astype(f32) + sums[3, k].astype(f32))
        )
        hidden_ref[k] = h
        squares = squares + h * h
    inv_rms = lax.rsqrt(jnp.sum(squares, axis=1, keepdims=True) * (1.0 / 4096.0) + norm_eps)
    for s in range(4):
        base = lax.rem(x + (4 - s), 4) * 2
        fa_ref[s] = (hidden_ref[base + c] * inv_rms * gain[base + c]).astype(bf16)
        other = base + 1 - c
        rows = (hidden_ref[other] * inv_rms * gain[other]).astype(bf16)
        for t in range(8):
            fb_ref[t, s] = rows


BLOCKS = 4
WIDTH = 512


def fetch(pieces, buffer, sems):
    copies = [
        [
            pltpu.make_async_copy(
                ref.at[pl.ds(lo, 256), pl.ds(j * WIDTH, WIDTH)],
                buffer.at[j, pl.ds(p * 256, 256)],
                sems.at[j, p],
            )
            for p, (ref, lo) in enumerate(pieces)
        ]
        for j in range(BLOCKS)
    ]
    for block in copies:
        for copy in block:
            copy.start()
    return copies


def lay_rows(rows_ref, parts):
    for to, take in parts:
        at = pl.ds(pl.multiple_of(to * 16, 16), 16)
        for k in range(4):
            rows_ref[at, k * 512 : k * 512 + 512] = take(k)


def first_kernel(at_ref, own, f1, f2, f3, g1, g2, g3, *refs):
    rows = refs[:8]
    out_ref, buffer, rows_ref, sems = refs[8:]
    pieces = [(own, 0), (own, 256), (f1, 0), (g1, 0), (f2, 0), (g2, 0), (f3, 0), (g3, 0)]
    copies = fetch(pieces, buffer, sems)
    z, y = at_ref[2], at_ref[3]
    parts = []
    for dz in range(8):
        for dy in range(4):
            to = lax.rem(z + (8 - dz), 8) * 4 + lax.rem(y + (4 - dy), 4)
            parts.append((to, functools.partial(lambda dz, dy, k: rows[dz][dy, k], dz, dy)))
    lay_rows(rows_ref, parts)
    for j in range(BLOCKS):
        for copy in copies[j]:
            copy.wait()
        out_ref[j] = jnp.dot(rows_ref[...], buffer[j], preferred_element_type=f32)


def second_kernel(at_ref, own, first, second, *refs):
    rows = refs[:4]
    part_ref, goal_ref, out_ref, buffer, rows_ref, sems = refs[4:]
    pieces = [(own, 0), (own, 256)]
    for s in range(3):
        pieces += [(first, s * 256), (second, s * 256)]
    copies = fetch(pieces, buffer, sems)
    y = at_ref[3]
    parts = []
    for dz in range(8):
        for dy in range(4):
            to = dz * 4 + lax.rem(y + (4 - dy), 4)
            parts.append((to, functools.partial(lambda dz, dy, k: rows[dy][dz, k], dz, dy)))
    lay_rows(rows_ref, parts)
    top = jnp.full((512, 1), -jnp.inf, f32)
    total = jnp.zeros((512, 1), f32)
    picked = jnp.zeros((512, 1), f32)
    goal = goal_ref[...]
    for j in range(BLOCKS):
        for copy in copies[j]:
            copy.wait()
        logits = part_ref[j] + jnp.dot(rows_ref[...], buffer[j], preferred_element_type=f32)
        column = lax.broadcasted_iota(i32, logits.shape, 1) + j * WIDTH
        new = jnp.maximum(top, jnp.max(logits, axis=1, keepdims=True))
        total = total * jnp.exp(top - new) + jnp.sum(
            jnp.exp(logits - new), axis=1, keepdims=True
        )
        picked = picked + jnp.sum(jnp.where(column == goal, logits, 0.0), axis=1, keepdims=True)
        top = new
    eye = lax.broadcasted_iota(i32, (128, 128), 0) == lax.broadcasted_iota(i32, (128, 128), 1)
    lines = []
    for values in (top + jnp.log(total), picked):
        for q in range(4):
            block = jnp.where(eye, values[q * 128 : q * 128 + 128], 0.0)
            lines.append(jnp.sum(block, axis=0, keepdims=True))
    lines = jnp.concatenate(lines, axis=0)
    for t in range(32):
        out_ref[t] = lines


def logits_call(kernel, at, weights, rest, out_shape):
    vmem = pl.BlockSpec(memory_space=pltpu.VMEM)
    return pl.pallas_call(
        kernel,
        out_shape=out_shape,
        in_specs=[pl.BlockSpec(memory_space=pltpu.SMEM)]
        + [pl.BlockSpec(memory_space=pltpu.HBM)] * len(weights)
        + [vmem] * len(rest),
        out_specs=vmem,
        scratch_shapes=[
            pltpu.VMEM((BLOCKS, 2048, WIDTH), bf16),
            pltpu.VMEM((512, 2048), bf16),
            pltpu.SemaphoreType.DMA((BLOCKS, 8)),
        ],
        cost_estimate=pl.CostEstimate(
            flops=2 * 512 * 2048 * 2048, bytes_accessed=12 << 20, transcendentals=0
        ),
        compiler_params=pltpu.CompilerParams(vmem_limit_bytes=40 << 20),
    )(at, *weights, *rest)


def merge_kernel(got_ref, label_ref, loss_ref, sums_ref):
    lse = [got_ref[k][:4] for k in range(32)]
    top = functools.reduce(jnp.maximum, lse)
    total = functools.reduce(lambda a, b: a + b, [jnp.exp(v - top) for v in lse])
    picked = functools.reduce(lambda a, b: a + b, [got_ref[k][4:] for k in range(32)])
    loss = top + jnp.log(total) - picked
    loss_ref[...] = loss
    domain = lax.broadcasted_iota(i32, (128, 128), 0)
    by_domain = jnp.zeros((128, 128), f32)
    for q in range(4):
        same = domain == label_ref[q : q + 1, :]
        by_domain = by_domain + jnp.where(same, loss[q : q + 1, :], 0.0)
    column = jnp.sum(by_domain, axis=1, keepdims=True)
    eye = domain == lax.broadcasted_iota(i32, (128, 128), 1)
    line = jnp.sum(jnp.where(eye, column, 0.0), axis=0, keepdims=True)
    for t in range(8):
        sums_ref[t] = jnp.broadcast_to(line, (8, 128))


def output_kernel(sums_ref, tally, prev, old, new_ref, probs_ref):
    sums = sums_ref[0]
    for t in range(1, 8):
        sums = sums + sums_ref[t]
    sums = sums[0:1]
    reward = sums / jnp.maximum(tally[...], 1.0) / prev[...]
    new = memory_rate * old[...] + (1.0 - memory_rate) * reward
    real = lax.broadcasted_iota(i32, (1, 128), 1) < DOMAINS
    scaled = jnp.where(real, step_rate * new, -jnp.inf)
    e = jnp.exp(scaled - jnp.max(scaled, axis=1, keepdims=True))
    soft = e / jnp.sum(e, axis=1, keepdims=True)
    new_ref[...] = new
    probs_ref[...] = (1.0 - DOMAINS * explore_mass) * soft + explore_mass


def program(
    embedded, targets, labels, counts, destinations, gain_in, w_query, w_key, w_value, w_out,
    gain_out, w_vocab, prev_probs, log_weights,
):
    z, y, x, c = (lax.axis_index(a) for a in ALL)
    d, m = z * NY + y, x * NC + c
    at = jnp.stack([x, c, z, y]).astype(i32)

    w_other = shift(w_vocab, "c", 1)
    rows = w_vocab[:256]
    w_first = [shift(rows, "x", s) for s in (1, 2, 3)]

    packed = call(
        pack_kernel, sds((32, 5, 8, 128), bf16),
        (embedded, targets, labels.reshape(1, 4), destinations.reshape(1, 4)),
        scratch=[pltpu.VMEM((8, 128), f32)],
    )
    got = lax.all_to_all(packed, DP, 0, 0, tiled=True)

    meta = got[:, 4]
    label_of = meta[:, 4, 0:4].reshape(128).astype(i32)
    goes_to = meta[:, 5, 0:4].reshape(128).astype(i32)
    slot = jnp.arange(128, dtype=i32)
    live = slot % 4 < jnp.repeat(counts, 4)
    chosen = live[None, :] & (goes_to[None, :] == jnp.arange(64, dtype=i32)[:, None])
    source_row = jnp.sum(jnp.where(chosen, (slot // 4) * 5 + slot % 4, 0), axis=1)
    picked = call(select_kernel, sds((64, 8, 128), bf16), (got.reshape(160, 8, 128),), source_row)
    block = lax.all_to_all(picked.reshape(32, 16, 128), DP, 0, 0, tiled=True)

    same = lax.all_gather(block, "x", axis=0, tiled=False)
    other = shift(same, "c", 1)

    cosine, sine = rope_tables()
    keep, send, resid = call(
        attention_kernel,
        [sds((4, 8, 16, 512), bf16), sds((4, 8, 16, 512), bf16), sds((8, 16, 512), bf16)],
        (
            same, other, gain_in.reshape(8, 1, 512), w_query, w_key, w_value, w_out,
            jnp.asarray(cosine), jnp.asarray(sine),
        ),
        at,
        scratch=[pltpu.VMEM((8, 16, 256), bf16)],
        flops=1 << 30,
    )
    got_part = shift(send, "c", 1)
    pair = call(pair_kernel, sds((4, 8, 16, 512), bf16), (keep, got_part))
    sums = lax.all_to_all(pair, "x", 0, 0, tiled=True)

    (_, first_w, own_w) = lax.optimization_barrier((pair, tuple(w_first), w_vocab))
    rows = own_w[256:]
    w_second = [shift(rows, "x", s) for s in (1, 2, 3)]
    w_first_other = shift(jnp.concatenate(first_w, axis=0), "c", 1)

    fa, fb = call(
        final_kernel, [sds((4, 16, 512), bf16), sds((8, 4, 16, 512), bf16)],
        (resid, sums, gain_out.reshape(8, 1, 512)), at,
        scratch=[pltpu.VMEM((8, 16, 512), f32)],
    )

    parts = [shift(fa, "y", s) for s in (1, 2, 3)]
    column = lax.all_to_all(fb, "z", 0, 0, tiled=True)
    group = jnp.stack([fa, *parts])
    up, down = [group], [group]
    for _ in range(3):
        up.append(shift(up[-1], "z", 1))
        down.append(shift(down[-1], "z", NZ - 1))
    rows_b = [column] + [shift(column, "y", s) for s in (1, 2, 3)]
    up.append(shift(up[-1], "z", 1))
    rows_a = [*up, down[3], down[2], down[1]]
    w_second_other = shift(jnp.concatenate(w_second, axis=0), "c", 1)

    seq_ids = jnp.dot(
        chosen.astype(bf16), meta[:, :4].reshape(128, 128), preferred_element_type=f32
    ).astype(i32)
    seq_goals = seq_ids[:, :64] * 256 + seq_ids[:, 64:]
    seq_labels = jnp.sum(jnp.where(chosen, label_of[None, :], 0), axis=1)
    mine = lax.dynamic_slice(
        seq_goals.reshape(32, 2, 4, 16), (0, m // 4, m % 4, 0), (32, 1, 1, 16)
    ).reshape(512)
    kinds = lax.dynamic_slice(seq_labels.reshape(32, 2), (0, m // 4), (32, 1))
    kinds = jnp.broadcast_to(kinds, (32, 16)).reshape(4, 128)
    goals = (mine - d * 2048).reshape(512, 1)
    domain = jnp.arange(128, dtype=i32)
    tally = SEQ_LEN * jnp.sum(
        (live[:, None] & (label_of[:, None] == domain[None, :])).astype(f32), axis=0
    )

    partial = logits_call(
        first_kernel, at, (w_vocab, *w_first, *w_second), rows_a,
        sds((BLOCKS, 512, WIDTH), f32),
    )
    pieces = logits_call(
        second_kernel, at, (w_other, w_first_other, w_second_other), (*rows_b, partial, goals),
        sds((32, 8, 128), f32),
    )
    merged = lax.all_to_all(pieces, DP, 0, 0, tiled=True)
    losses, sums_here = call(
        merge_kernel, [sds((4, 128), f32), sds((8, 8, 128), f32)], (merged, kinds)
    )
    own_loss = lax.dynamic_slice_in_dim(losses.reshape(512), d * 16, 16, 0)
    all_sums = lax.all_to_all(sums_here, MP, 0, 0, tiled=True)
    line = lambda v, fill: jnp.pad(v, (0, 128 - DOMAINS), constant_values=fill).reshape(1, 128)
    new_weights, probs = call(
        output_kernel, [sds((1, 128), f32)] * 2,
        (all_sums, tally.reshape(1, 128), line(prev_probs, 1.0), line(log_weights, 0.0)),
    )
    return own_loss, new_weights[0, :DOMAINS], probs[0, :DOMAINS]


def solution(mesh):
    torus = Mesh(mesh.devices.reshape(NZ, NY, NX, NC), ALL)
    in_specs = (
        P(DP, None, MP), P(DP, None), P(DP), P(), P(DP), P(), P(None, MP), P(None, MP),
        P(None, MP), P(MP, None), P(), P(MP, DP), P(), P(),
    )
    return jax.shard_map(
        program, mesh=torus, in_specs=in_specs, out_specs=(P(ALL), P(), P()), check_vma=False
    )
```

```python
import functools

import jax
import jax.numpy as jnp
import numpy as np
from jax import lax
from jax.experimental import pallas as pl
from jax.experimental.pallas import tpu as pltpu
from jax.sharding import Mesh
from jax.sharding import PartitionSpec as P


HEAD_DIM = 128
DOMAINS = 22
SEQ_LEN = 64
DP = ("z", "y")
MP = ("x", "c")
ALL = ("z", "y", "x", "c")
NZ, NY, NX, NC = 8, 4, 4, 2

norm_eps = 1e-05
rope_base = 500000.0
memory_rate = 0.9
step_rate = 0.02
explore_mass = 0.005


bf16 = jnp.bfloat16
f32 = jnp.float32
i32 = jnp.int32


def shift(array, axis, by):
    n = {"z": NZ, "y": NY, "x": NX, "c": NC}[axis]
    return lax.ppermute(array, axis, [(i, (i + by) % n) for i in range(n)])


def call(kernel, out_shape, args, scalars=None, scratch=(), flops=0, vmem=None):
    spec = pl.BlockSpec(memory_space=pltpu.VMEM)
    many = isinstance(out_shape, (list, tuple))
    params = {} if vmem is None else {"vmem_limit_bytes": vmem}
    return pl.pallas_call(
        kernel,
        out_shape=out_shape,
        in_specs=([pl.BlockSpec(memory_space=pltpu.SMEM)] if scalars is not None else [])
        + [spec] * len(args),
        out_specs=[spec] * len(out_shape) if many else spec,
        scratch_shapes=scratch,
        compiler_params=pltpu.CompilerParams(**params),
        cost_estimate=pl.CostEstimate(flops=flops, bytes_accessed=0, transcendentals=0)
        if flops
        else None,
    )(*(() if scalars is None else (scalars,)), *args)


def sds(shape, dtype):
    return jax.ShapeDtypeStruct(shape, dtype)


def pack_kernel(embedded, targets, labels, destinations, out_ref, meta_ref):
    ids = targets[...]
    meta_ref[...] = jnp.zeros((8, 128), f32)
    meta_ref[0:4, 0:64] = (ids // 256).astype(f32)
    meta_ref[0:4, 64:128] = (ids % 256).astype(f32)
    meta_ref[4:5, 0:4] = labels[...].astype(f32)
    meta_ref[5:6, 0:4] = destinations[...].astype(f32)
    meta = meta_ref[...].astype(bf16)
    for r in range(8):
        for col in range(4):
            for s in range(4):
                out_ref[r * 4 + col, s] = embedded[
                    s, r * 8 : r * 8 + 8, col * 128 : col * 128 + 128
                ]
            out_ref[r * 4 + col, 4] = meta


def select_kernel(row_ref, got_ref, out_ref):
    for g in range(64):
        out_ref[g] = got_ref[row_ref[g]]


def rope_tables():
    half = HEAD_DIM // 2
    frequency = np.power(rope_base, -np.arange(half) * 2.0 / HEAD_DIM)
    angle = np.arange(SEQ_LEN)[:, None] * frequency[None, :]
    cosine = np.concatenate([np.cos(angle), np.cos(angle)], axis=1)
    sine = np.concatenate([-np.sin(angle), np.sin(angle)], axis=1)
    both = [np.concatenate([t, t], axis=0).astype(np.float32) for t in (cosine, sine)]
    return both


def attention_kernel(
    at_ref, same, other, gain, wq, wk, wv, wo, cos, sin, keep_ref, send_ref, resid_ref, mixed_ref
):
    x, c = at_ref[0], at_ref[1]
    m = x * 2 + c
    blocks = [same.at[t] for t in range(4)] + [other.at[t] for t in range(4)]

    def feature_block(k):
        return (k % 4) * 2 + (c if k < 4 else 1 - c)

    def piece(ref, col):
        return jnp.concatenate([ref[r * 4 + col] for r in range(8)], axis=0).astype(f32)

    squares = jnp.zeros((128, 128), f32)
    for ref in blocks:
        for col in range(4):
            v = piece(ref, col)
            squares = squares + v * v
    inv_rms = lax.rsqrt(jnp.sum(squares, axis=1, keepdims=True) * (1.0 / 4096.0) + norm_eps)

    query = jnp.zeros((128, 256), f32)
    key = jnp.zeros((128, 128), f32)
    value = jnp.zeros((128, 128), f32)
    for k, ref in enumerate(blocks):
        fb = feature_block(k)
        g = gain[fb]
        normed = jnp.concatenate(
            [
                (piece(ref, col) * inv_rms * g[:, col * 128 : col * 128 + 128]).astype(bf16)
                for col in range(4)
            ],
            axis=1,
        )
        rows = pl.ds(pl.multiple_of(fb * 512, 512), 512)
        query = query + jnp.dot(normed, wq[rows, :], preferred_element_type=f32)
        key = key + jnp.dot(normed, wk[rows, :], preferred_element_type=f32)
        value = value + jnp.dot(normed, wv[rows, :], preferred_element_type=f32)

    def in_order(t):
        return jnp.concatenate(
            [t[r * 16 + s * 8 : r * 16 + s * 8 + 8] for s in range(2) for r in range(8)], axis=0
        )

    cosine, sine = cos[...], sin[...]

    def rotated(t):
        return (t * cosine + pltpu.roll(t, 64, axis=1) * sine).astype(bf16)

    query, key, value = in_order(query), rotated(in_order(key)), in_order(value).astype(bf16)
    row = lax.broadcasted_iota(i32, (128, 128), 0)
    column = lax.broadcasted_iota(i32, (128, 128), 1)
    seen = (row // SEQ_LEN == column // SEQ_LEN) & (column <= row)
    for h in range(2):
        q = rotated(query[:, h * 128 : h * 128 + 128])
        scores = lax.dot_general(q, key, (((1,), (1,)), ((), ())), preferred_element_type=f32)
        scores = jnp.where(seen, scores * HEAD_DIM ** (-0.5), -jnp.inf)
        top = jnp.max(scores, axis=1, keepdims=True)
        e = jnp.exp(scores - top)
        weights = (e / jnp.sum(e, axis=1, keepdims=True)).astype(bf16)
        mixed = jnp.dot(weights, value, preferred_element_type=f32).astype(bf16)
        mixed_ref[:, :, h * 128 : h * 128 + 128] = mixed.reshape(8, 16, 128)
    left = jnp.concatenate(
        [mixed_ref[t * 2 + c] for t in range(4)] + [mixed_ref[t * 2 + 1 - c] for t in range(4)],
        axis=0,
    )
    for fb in range(8):
        part = jnp.dot(left, wo[:, fb * 512 : fb * 512 + 512], preferred_element_type=f32)
        part = part.astype(bf16).reshape(8, 16, 512)
        keep_ref[:, fb] = part[:4]
        send_ref[:, fb] = part[4:]

    first = m < 4
    r0 = lax.rem(m, 4) * 2
    for k, ref in enumerate(blocks):
        fb = feature_block(k)
        rows = []
        for r in range(2):
            cols = []
            for col in range(4):
                v = ref[(r0 + r) * 4 + col].astype(f32)
                cols.append(jnp.where(first, v[:8], v[8:]))
            rows.append(jnp.concatenate(cols, axis=1))
        resid_ref[fb] = jnp.concatenate(rows, axis=0).astype(bf16)


def pair_kernel(keep_ref, got_ref, out_ref):
    out_ref[...] = (keep_ref[...].astype(f32) + got_ref[...].astype(f32)).astype(bf16)


def final_kernel(at_ref, resid, sums, gain, fa_ref, fb_ref, hidden_ref):
    x, c = at_ref[0], at_ref[1]
    squares = jnp.zeros((16, 512), f32)
    for k in range(8):
        h = resid[k].astype(f32) + (
            (sums[0, k].astype(f32) + sums[1, k].astype(f32))
            + (sums[2, k].astype(f32) + sums[3, k].astype(f32))
        )
        hidden_ref[k] = h
        squares = squares + h * h
    inv_rms = lax.rsqrt(jnp.sum(squares, axis=1, keepdims=True) * (1.0 / 4096.0) + norm_eps)
    for s in range(4):
        base = lax.rem(x + (4 - s), 4) * 2
        fa_ref[s] = (hidden_ref[base + c] * inv_rms * gain[base + c]).astype(bf16)
        other = base + 1 - c
        rows = (hidden_ref[other] * inv_rms * gain[other]).astype(bf16)
        for t in range(8):
            fb_ref[t, s] = rows


BLOCKS = 4
WIDTH = 512


FIRST = 192


def logits_kernel(at_ref, *refs):
    own, f1, f2, f3, g1, g2, g3, w_other, first, second = refs[:10]
    rows_a, rows_b = refs[10:18], refs[18:22]
    goal_ref, out_ref, buffer, rows_ref, top_ref, sum_ref, pick_ref, sems = refs[22:]
    late = 512 - FIRST
    pieces = []
    for f, g in ((own, own), (f1, g1), (f2, g2), (f3, g3)):
        pieces += [(f, 0, FIRST), (g, FIRST if g is own else 0, late)]
    pieces += [(w_other, 0, FIRST), (w_other, FIRST, late)]
    for s in range(3):
        pieces += [(first, s * FIRST, FIRST), (second, s * late, late)]

    def copies(j):
        found, at = [], 0
        for p, (ref, lo, n) in enumerate(pieces):
            found.append(
                pltpu.make_async_copy(
                    ref.at[pl.ds(lo, n), pl.ds(pl.multiple_of(j * WIDTH, WIDTH), WIDTH)],
                    buffer.at[j, pl.ds(at, n)],
                    sems.at[j, p],
                )
            )
            at += n
        return found

    @pl.loop(0, BLOCKS)
    def _(j):
        for copy in copies(j):
            copy.start()

    z, y = at_ref[2], at_ref[3]
    for dz in range(8):
        for dy in range(4):
            in_y = lax.rem(y + (4 - dy), 4)
            a_rows = pl.ds(pl.multiple_of((lax.rem(z + (8 - dz), 8) * 4 + in_y) * 16, 16), 16)
            b_rows = pl.ds(pl.multiple_of((dz * 4 + in_y) * 16, 16), 16)
            for k in range(4):
                rows_ref[a_rows, k * 512 : k * 512 + 512] = rows_a[dz][dy, k]
                rows_ref[b_rows, 2048 + k * 512 : 2048 + k * 512 + 512] = rows_b[dy][dz, k]
    top_ref[...] = jnp.full((512, 1), -jnp.inf, f32)
    sum_ref[...] = jnp.zeros((512, 1), f32)
    pick_ref[...] = jnp.zeros((512, 1), f32)

    @pl.loop(0, BLOCKS)
    def _(j):
        for copy in copies(j):
            copy.wait()
        logits = jnp.dot(rows_ref[...], buffer[j], preferred_element_type=f32)
        column = lax.broadcasted_iota(i32, logits.shape, 1)
        top = top_ref[...]
        new = jnp.maximum(top, jnp.max(logits, axis=1, keepdims=True))
        sum_ref[...] = sum_ref[...] * jnp.exp(top - new) + jnp.sum(
            jnp.exp(logits - new), axis=1, keepdims=True
        )
        hit = column == goal_ref[...] - j * WIDTH
        pick_ref[...] += jnp.sum(jnp.where(hit, logits, 0.0), axis=1, keepdims=True)
        top_ref[...] = new

    eye = lax.broadcasted_iota(i32, (128, 128), 0) == lax.broadcasted_iota(i32, (128, 128), 1)
    lines = []
    for values in (top_ref[...] + jnp.log(sum_ref[...]), pick_ref[...]):
        for q in range(4):
            block = jnp.where(eye, values[q * 128 : q * 128 + 128], 0.0)
            lines.append(jnp.sum(block, axis=0, keepdims=True))
    lines = jnp.concatenate(lines, axis=0)
    for t in range(32):
        out_ref[t] = lines


def logits_call(at, weights, rest):
    vmem = pl.BlockSpec(memory_space=pltpu.VMEM)
    return pl.pallas_call(
        logits_kernel,
        out_shape=sds((32, 8, 128), f32),
        in_specs=[pl.BlockSpec(memory_space=pltpu.SMEM)]
        + [pl.BlockSpec(memory_space=pltpu.HBM)] * len(weights)
        + [vmem] * len(rest),
        out_specs=vmem,
        scratch_shapes=[
            pltpu.VMEM((BLOCKS, 4096, WIDTH), bf16),
            pltpu.VMEM((512, 4096), bf16),
            pltpu.VMEM((512, 1), f32),
            pltpu.VMEM((512, 1), f32),
            pltpu.VMEM((512, 1), f32),
            pltpu.SemaphoreType.DMA((BLOCKS, 16)),
        ],
        name="logits",
        cost_estimate=pl.CostEstimate(
            flops=2 * 512 * 4096 * 2048, bytes_accessed=20 << 20, transcendentals=0
        ),
        compiler_params=pltpu.CompilerParams(vmem_limit_bytes=44 << 20),
    )(at, *weights, *rest)


def merge_kernel(got_ref, label_ref, loss_ref, sums_ref):
    lse = [got_ref[k][:4] for k in range(32)]
    top = functools.reduce(jnp.maximum, lse)
    total = functools.reduce(lambda a, b: a + b, [jnp.exp(v - top) for v in lse])
    picked = functools.reduce(lambda a, b: a + b, [got_ref[k][4:] for k in range(32)])
    loss = top + jnp.log(total) - picked
    loss_ref[...] = loss
    domain = lax.broadcasted_iota(i32, (128, 128), 0)
    by_domain = jnp.zeros((128, 128), f32)
    for q in range(4):
        same = domain == label_ref[q : q + 1, :]
        by_domain = by_domain + jnp.where(same, loss[q : q + 1, :], 0.0)
    column = jnp.sum(by_domain, axis=1, keepdims=True)
    eye = domain == lax.broadcasted_iota(i32, (128, 128), 1)
    line = jnp.sum(jnp.where(eye, column, 0.0), axis=0, keepdims=True)
    for t in range(8):
        sums_ref[t] = jnp.broadcast_to(line, (8, 128))


def output_kernel(sums_ref, tally, prev, old, new_ref, probs_ref):
    sums = sums_ref[0]
    for t in range(1, 8):
        sums = sums + sums_ref[t]
    sums = sums[0:1]
    reward = sums / jnp.maximum(tally[...], 1.0) / prev[...]
    new = memory_rate * old[...] + (1.0 - memory_rate) * reward
    real = lax.broadcasted_iota(i32, (1, 128), 1) < DOMAINS
    scaled = jnp.where(real, step_rate * new, -jnp.inf)
    e = jnp.exp(scaled - jnp.max(scaled, axis=1, keepdims=True))
    soft = e / jnp.sum(e, axis=1, keepdims=True)
    new_ref[...] = new[:, :DOMAINS]
    probs_ref[...] = ((1.0 - DOMAINS * explore_mass) * soft + explore_mass)[:, :DOMAINS]


def program(
    embedded, targets, labels, counts, destinations, gain_in, w_query, w_key, w_value, w_out,
    gain_out, w_vocab, prev_probs, log_weights,
):
    z, y, x, c = (lax.axis_index(a) for a in ALL)
    d, m = z * NY + y, x * NC + c
    at = jnp.stack([x, c, z, y]).astype(i32)

    w_other = shift(w_vocab, "c", 1)
    rows = w_vocab[:FIRST]
    w_first = [shift(rows, "x", s) for s in (1, 2, 3)]

    packed = call(
        pack_kernel, sds((32, 5, 8, 128), bf16),
        (embedded, targets, labels.reshape(1, 4), destinations.reshape(1, 4)),
        scratch=[pltpu.VMEM((8, 128), f32)],
    )
    got = lax.all_to_all(packed, DP, 0, 0, tiled=True)

    meta = got[:, 4]
    label_of = meta[:, 4, 0:4].reshape(128).astype(i32)
    goes_to = meta[:, 5, 0:4].reshape(128).astype(i32)
    slot = jnp.arange(128, dtype=i32)
    live = slot % 4 < jnp.repeat(counts, 4)
    chosen = live[None, :] & (goes_to[None, :] == jnp.arange(64, dtype=i32)[:, None])
    source_row = jnp.sum(jnp.where(chosen, (slot // 4) * 5 + slot % 4, 0), axis=1)
    picked = call(select_kernel, sds((64, 8, 128), bf16), (got.reshape(160, 8, 128),), source_row)
    block = lax.all_to_all(picked.reshape(32, 16, 128), DP, 0, 0, tiled=True)

    same = lax.all_gather(block, "x", axis=0, tiled=False)
    other = shift(same, "c", 1)

    cosine, sine = rope_tables()
    keep, send, resid = call(
        attention_kernel,
        [sds((4, 8, 16, 512), bf16), sds((4, 8, 16, 512), bf16), sds((8, 16, 512), bf16)],
        (
            same, other, gain_in.reshape(8, 1, 512), w_query, w_key, w_value, w_out,
            jnp.asarray(cosine), jnp.asarray(sine),
        ),
        at,
        scratch=[pltpu.VMEM((8, 16, 256), bf16)],
        flops=1 << 30,
    )
    got_part = shift(send, "c", 1)
    pair = call(pair_kernel, sds((4, 8, 16, 512), bf16), (keep, got_part))
    sums = lax.all_to_all(pair, "x", 0, 0, tiled=True)

    (_, first_w, own_w) = lax.optimization_barrier((pair, tuple(w_first), w_vocab))
    rows = own_w[FIRST:]
    w_second = [shift(rows, "x", s) for s in (1, 2, 3)]
    w_first_other = shift(jnp.concatenate(first_w, axis=0), "c", 1)

    seq_ids = jnp.dot(
        chosen.astype(bf16), meta[:, :4].reshape(128, 128), preferred_element_type=f32
    ).astype(i32)
    seq_goals = seq_ids[:, :64] * 256 + seq_ids[:, 64:]
    seq_labels = jnp.sum(jnp.where(chosen, label_of[None, :], 0), axis=1)
    mine = lax.dynamic_slice(
        seq_goals.reshape(32, 2, 4, 16), (0, m // 4, m % 4, 0), (32, 1, 1, 16)
    ).reshape(512)
    kinds = lax.dynamic_slice(seq_labels.reshape(32, 2), (0, m // 4), (32, 1))
    kinds = jnp.broadcast_to(kinds, (32, 16)).reshape(4, 128)
    goals = (mine - d * 2048).reshape(512, 1)
    domain = jnp.arange(128, dtype=i32)
    tally = SEQ_LEN * jnp.sum(
        (live[:, None] & (label_of[:, None] == domain[None, :])).astype(f32), axis=0
    )
    sums, goals = lax.optimization_barrier((sums, goals))

    fa, fb = call(
        final_kernel, [sds((4, 16, 512), bf16), sds((8, 4, 16, 512), bf16)],
        (resid, sums, gain_out.reshape(8, 1, 512)), at,
        scratch=[pltpu.VMEM((8, 16, 512), f32)],
    )

    parts = [shift(fa, "y", s) for s in (1, 2, 3)]
    column = lax.all_to_all(fb, "z", 0, 0, tiled=True)
    group = jnp.stack([fa, *parts])
    up, down = [group], [group]
    for _ in range(3):
        up.append(shift(up[-1], "z", 1))
        down.append(shift(down[-1], "z", NZ - 1))
    rows_b = [column] + [shift(column, "y", s) for s in (1, 2, 3)]
    up.append(shift(up[-1], "z", 1))
    rows_a = [*up, down[3], down[2], down[1]]
    w_second_other = shift(jnp.concatenate(w_second, axis=0), "c", 1)

    pieces = logits_call(
        at, (w_vocab, *w_first, *w_second, w_other, w_first_other, w_second_other),
        (*rows_a, *rows_b, goals),
    )
    merged = lax.all_to_all(pieces, DP, 0, 0, tiled=True)
    losses, sums_here = call(
        merge_kernel, [sds((4, 128), f32), sds((8, 8, 128), f32)], (merged, kinds)
    )
    own_loss = lax.dynamic_slice_in_dim(losses.reshape(512), d * 16, 16, 0)
    all_sums = lax.all_to_all(sums_here, MP, 0, 0, tiled=True)
    line = lambda v, fill: jnp.pad(v, (0, 128 - DOMAINS), constant_values=fill).reshape(1, 128)
    new_weights, probs = call(
        output_kernel, [sds((1, DOMAINS), f32)] * 2,
        (all_sums, tally.reshape(1, 128), line(prev_probs, 1.0), line(log_weights, 0.0)),
    )
    return own_loss, new_weights.reshape(DOMAINS), probs.reshape(DOMAINS)


def solution(mesh):
    torus = Mesh(mesh.devices.reshape(NZ, NY, NX, NC), ALL)
    in_specs = (
        P(DP, None, MP), P(DP, None), P(DP), P(), P(DP), P(), P(None, MP), P(None, MP),
        P(None, MP), P(MP, None), P(), P(MP, DP), P(), P(),
    )
    return jax.shard_map(
        program, mesh=torus, in_specs=in_specs, out_specs=(P(ALL), P(), P()), check_vma=False
    )
```

```python
import functools

import jax
import jax.numpy as jnp
import numpy as np
from jax import lax
from jax.experimental import pallas as pl
from jax.experimental.pallas import tpu as pltpu
from jax.sharding import Mesh
from jax.sharding import PartitionSpec as P


HEAD_DIM = 128
DOMAINS = 22
SEQ_LEN = 64
DP = ("z", "y")
MP = ("x", "c")
ALL = ("z", "y", "x", "c")
NZ, NY, NX, NC = 8, 4, 4, 2

norm_eps = 1e-05
rope_base = 500000.0
memory_rate = 0.9
step_rate = 0.02
explore_mass = 0.005


bf16 = jnp.bfloat16
f32 = jnp.float32
i32 = jnp.int32


def shift(array, axis, by):
    n = {"z": NZ, "y": NY, "x": NX, "c": NC}[axis]
    return lax.ppermute(array, axis, [(i, (i + by) % n) for i in range(n)])


def call(kernel, out_shape, args, scalars=None, scratch=(), flops=0, vmem=None):
    spec = pl.BlockSpec(memory_space=pltpu.VMEM)
    many = isinstance(out_shape, (list, tuple))
    params = {} if vmem is None else {"vmem_limit_bytes": vmem}
    return pl.pallas_call(
        kernel,
        out_shape=out_shape,
        in_specs=([pl.BlockSpec(memory_space=pltpu.SMEM)] if scalars is not None else [])
        + [spec] * len(args),
        out_specs=[spec] * len(out_shape) if many else spec,
        scratch_shapes=scratch,
        compiler_params=pltpu.CompilerParams(**params),
        cost_estimate=pl.CostEstimate(flops=flops, bytes_accessed=0, transcendentals=0)
        if flops
        else None,
    )(*(() if scalars is None else (scalars,)), *args)


def sds(shape, dtype):
    return jax.ShapeDtypeStruct(shape, dtype)


def pack_kernel(embedded, targets, labels, destinations, out_ref, meta_ref):
    ids = targets[...]
    meta_ref[...] = jnp.zeros((8, 128), f32)
    meta_ref[0:4, 0:64] = (ids // 256).astype(f32)
    meta_ref[0:4, 64:128] = (ids % 256).astype(f32)
    meta_ref[4:5, 0:4] = labels[...].astype(f32)
    meta_ref[5:6, 0:4] = destinations[...].astype(f32)
    meta = meta_ref[...].astype(bf16)
    for r in range(8):
        for col in range(4):
            for s in range(4):
                out_ref[r * 4 + col, s] = embedded[
                    s, r * 8 : r * 8 + 8, col * 128 : col * 128 + 128
                ]
            out_ref[r * 4 + col, 4] = meta


def select_kernel(row_ref, got_ref, out_ref):
    for g in range(64):
        out_ref[g] = got_ref[row_ref[g]]


def rope_tables():
    half = HEAD_DIM // 2
    frequency = np.power(rope_base, -np.arange(half) * 2.0 / HEAD_DIM)
    angle = np.arange(SEQ_LEN)[:, None] * frequency[None, :]
    cosine = np.concatenate([np.cos(angle), np.cos(angle)], axis=1)
    sine = np.concatenate([-np.sin(angle), np.sin(angle)], axis=1)
    both = [np.concatenate([t, t], axis=0).astype(np.float32) for t in (cosine, sine)]
    return both


def attention_kernel(
    at_ref, same, other, gain, wq, wk, wv, wo, cos, sin, keep_ref, send_ref, resid_ref, mixed_ref
):
    x, c = at_ref[0], at_ref[1]
    m = x * 2 + c
    blocks = [same.at[t] for t in range(4)] + [other.at[t] for t in range(4)]

    def feature_block(k):
        return (k % 4) * 2 + (c if k < 4 else 1 - c)

    def piece(ref, col):
        return jnp.concatenate([ref[r * 4 + col] for r in range(8)], axis=0).astype(f32)

    squares = jnp.zeros((128, 128), f32)
    for ref in blocks:
        for col in range(4):
            v = piece(ref, col)
            squares = squares + v * v
    inv_rms = lax.rsqrt(jnp.sum(squares, axis=1, keepdims=True) * (1.0 / 4096.0) + norm_eps)

    query = jnp.zeros((128, 256), f32)
    key = jnp.zeros((128, 128), f32)
    value = jnp.zeros((128, 128), f32)
    for k, ref in enumerate(blocks):
        fb = feature_block(k)
        g = gain[fb]
        normed = jnp.concatenate(
            [
                (piece(ref, col) * inv_rms * g[:, col * 128 : col * 128 + 128]).astype(bf16)
                for col in range(4)
            ],
            axis=1,
        )
        rows = pl.ds(pl.multiple_of(fb * 512, 512), 512)
        query = query + jnp.dot(normed, wq[rows, :], preferred_element_type=f32)
        key = key + jnp.dot(normed, wk[rows, :], preferred_element_type=f32)
        value = value + jnp.dot(normed, wv[rows, :], preferred_element_type=f32)

    def in_order(t):
        return jnp.concatenate(
            [t[r * 16 + s * 8 : r * 16 + s * 8 + 8] for s in range(2) for r in range(8)], axis=0
        )

    cosine, sine = cos[...], sin[...]

    def rotated(t):
        return (t * cosine + pltpu.roll(t, 64, axis=1) * sine).astype(bf16)

    query, key, value = in_order(query), rotated(in_order(key)), in_order(value).astype(bf16)
    row = lax.broadcasted_iota(i32, (128, 128), 0)
    column = lax.broadcasted_iota(i32, (128, 128), 1)
    seen = (row // SEQ_LEN == column // SEQ_LEN) & (column <= row)
    for h in range(2):
        q = rotated(query[:, h * 128 : h * 128 + 128])
        scores = lax.dot_general(q, key, (((1,), (1,)), ((), ())), preferred_element_type=f32)
        scores = jnp.where(seen, scores * HEAD_DIM ** (-0.5), -jnp.inf)
        top = jnp.max(scores, axis=1, keepdims=True)
        e = jnp.exp(scores - top)
        weights = (e / jnp.sum(e, axis=1, keepdims=True)).astype(bf16)
        mixed = jnp.dot(weights, value, preferred_element_type=f32).astype(bf16)
        mixed_ref[:, :, h * 128 : h * 128 + 128] = mixed.reshape(8, 16, 128)
    left = jnp.concatenate(
        [mixed_ref[t * 2 + c] for t in range(4)] + [mixed_ref[t * 2 + 1 - c] for t in range(4)],
        axis=0,
    )
    for fb in range(8):
        part = jnp.dot(left, wo[:, fb * 512 : fb * 512 + 512], preferred_element_type=f32)
        part = part.astype(bf16).reshape(8, 16, 512)
        keep_ref[:, fb] = part[:4]
        send_ref[:, fb] = part[4:]

    first = m < 4
    r0 = lax.rem(m, 4) * 2
    for k, ref in enumerate(blocks):
        fb = feature_block(k)
        rows = []
        for r in range(2):
            cols = []
            for col in range(4):
                v = ref[(r0 + r) * 4 + col].astype(f32)
                cols.append(jnp.where(first, v[:8], v[8:]))
            rows.append(jnp.concatenate(cols, axis=1))
        resid_ref[fb] = jnp.concatenate(rows, axis=0).astype(bf16)


def pair_kernel(keep_ref, got_ref, out_ref):
    out_ref[...] = (keep_ref[...].astype(f32) + got_ref[...].astype(f32)).astype(bf16)


def final_kernel(at_ref, resid, sums, gain, fa_ref, fb_ref, hidden_ref):
    x, c = at_ref[0], at_ref[1]
    squares = jnp.zeros((16, 512), f32)
    for k in range(8):
        h = resid[k].astype(f32) + (
            (sums[0, k].astype(f32) + sums[1, k].astype(f32))
            + (sums[2, k].astype(f32) + sums[3, k].astype(f32))
        )
        hidden_ref[k] = h
        squares = squares + h * h
    inv_rms = lax.rsqrt(jnp.sum(squares, axis=1, keepdims=True) * (1.0 / 4096.0) + norm_eps)
    for s in range(4):
        base = lax.rem(x + (4 - s), 4) * 2
        fa_ref[s] = (hidden_ref[base + c] * inv_rms * gain[base + c]).astype(bf16)
        other = base + 1 - c
        rows = (hidden_ref[other] * inv_rms * gain[other]).astype(bf16)
        for t in range(8):
            fb_ref[t, s] = rows


BLOCKS = 4
WIDTH = 512


FRONT = 256


def logits_kernel(at_ref, *refs):
    pieces, rows, goal_ref = refs[:14], refs[14:26], refs[26]
    (out_ref, buffer, stage_ref, rows_ref, logit_ref, top_ref, sum_ref, pick_ref, goals_ref,
     sems, row_sems) = refs[27:]
    whole, starts, at = (0, 7), [], 0
    for p in range(14):
        starts.append(at)
        at += 512 if p in whole else 256

    def copies(j):
        column = pl.ds(pl.multiple_of(j * WIDTH, WIDTH), WIDTH)
        return [
            pltpu.make_async_copy(
                ref.at[:, column],
                buffer.at[j, pl.ds(starts[p], 512 if p in whole else 256)],
                sems.at[j, p],
            )
            for p, ref in enumerate(pieces)
        ]

    row_copies = [
        pltpu.make_async_copy(ref, stage_ref.at[pl.ds(k * 256, 256)], row_sems.at[k])
        for k, ref in enumerate(rows[:8])
    ] + [
        pltpu.make_async_copy(ref, stage_ref.at[pl.ds(2048 + k * 512, 512)], row_sems.at[8 + k])
        for k, ref in enumerate(rows[8:])
    ]
    for copy in row_copies:
        copy.start()

    @pl.loop(0, BLOCKS)
    def _(j):
        for copy in copies(j):
            copy.start()

    eye = lax.broadcasted_iota(i32, (128, 128), 0) == lax.broadcasted_iota(i32, (128, 128), 1)
    for q in range(4):
        goals_ref[q * 128 : q * 128 + 128] = jnp.sum(
            jnp.where(eye, goal_ref[q : q + 1], 0.0), axis=1, keepdims=True
        )
    top_ref[...] = jnp.full((512, 1), -jnp.inf, f32)
    sum_ref[...] = jnp.zeros((512, 1), f32)
    pick_ref[...] = jnp.zeros((512, 1), f32)

    for copy in row_copies:
        copy.wait()
    z, y = at_ref[2], at_ref[3]
    for dz in range(8):
        for dy in range(4):
            in_y = lax.rem(y + (4 - dy), 4)
            a_rows = pl.ds(pl.multiple_of((lax.rem(z + (8 - dz), 8) * 4 + in_y) * 16, 16), 16)
            b_rows = pl.ds(pl.multiple_of((dz * 4 + in_y) * 16, 16), 16)
            for k in range(4):
                lo = dz * 256 + (dy * 4 + k) * 16
                rows_ref[a_rows, k * 512 : k * 512 + 512] = stage_ref[lo : lo + 16]
                lo = 2048 + dy * 512 + (dz * 4 + k) * 16
                rows_ref[b_rows, 2048 + k * 512 : 2560 + k * 512] = stage_ref[lo : lo + 16]

    def multiply(j):
        for copy in copies(j):
            copy.wait()
        return jnp.dot(rows_ref[...], buffer[j], preferred_element_type=f32)

    def reduce(j, logits):
        column = lax.broadcasted_iota(i32, logits.shape, 1).astype(f32)
        top = top_ref[...]
        new = jnp.maximum(top, jnp.max(logits, axis=1, keepdims=True))
        sum_ref[...] = sum_ref[...] * jnp.exp(top - new) + jnp.sum(
            jnp.exp(logits - new), axis=1, keepdims=True
        )
        hit = column == goals_ref[...] - lax.convert_element_type(j * WIDTH, f32)
        pick_ref[...] += jnp.sum(jnp.where(hit, logits, 0.0), axis=1, keepdims=True)
        top_ref[...] = new

    logit_ref[0] = multiply(0)

    @pl.loop(1, BLOCKS)
    def _(j):
        reduce(j - 1, logit_ref[lax.rem(j - 1, 2)])
        logit_ref[lax.rem(j, 2)] = multiply(j)

    reduce(jnp.int32(BLOCKS - 1), logit_ref[(BLOCKS - 1) % 2])
    lines = []
    for values in (top_ref[...] + jnp.log(sum_ref[...]), pick_ref[...]):
        for q in range(4):
            block = jnp.where(eye, values[q * 128 : q * 128 + 128], 0.0)
            lines.append(jnp.sum(block, axis=0, keepdims=True))
    lines = jnp.concatenate(lines, axis=0)
    for t in range(32):
        out_ref[t] = lines


def logits_call(at, weights, rows, goals):
    vmem = pl.BlockSpec(memory_space=pltpu.VMEM)
    hbm = pl.BlockSpec(memory_space=pltpu.HBM)
    rows = [r.reshape(-1, 512) for r in rows]
    return pl.pallas_call(
        logits_kernel,
        out_shape=sds((32, 8, 128), f32),
        in_specs=[pl.BlockSpec(memory_space=pltpu.SMEM)]
        + [hbm] * (len(weights) + len(rows))
        + [vmem],
        out_specs=vmem,
        scratch_shapes=[
            pltpu.VMEM((BLOCKS, 4096, WIDTH), bf16),
            pltpu.VMEM((4096, 512), bf16),
            pltpu.VMEM((512, 4096), bf16),
            pltpu.VMEM((2, 512, WIDTH), f32),
            pltpu.VMEM((512, 1), f32),
            pltpu.VMEM((512, 1), f32),
            pltpu.VMEM((512, 1), f32),
            pltpu.VMEM((512, 1), f32),
            pltpu.SemaphoreType.DMA((BLOCKS, 14)),
            pltpu.SemaphoreType.DMA((12,)),
        ],
        name="logits",
        cost_estimate=pl.CostEstimate(
            flops=2 * 512 * 4096 * 2048, bytes_accessed=20 << 20, transcendentals=0
        ),
        compiler_params=pltpu.CompilerParams(vmem_limit_bytes=36 << 20),
    )(at, *weights, *rows, goals)


def merge_kernel(got_ref, label_ref, loss_ref, sums_ref):
    lse = [got_ref[k][:4] for k in range(32)]
    top = functools.reduce(jnp.maximum, lse)
    total = functools.reduce(lambda a, b: a + b, [jnp.exp(v - top) for v in lse])
    picked = functools.reduce(lambda a, b: a + b, [got_ref[k][4:] for k in range(32)])
    loss = top + jnp.log(total) - picked
    loss_ref[...] = loss
    domain = lax.broadcasted_iota(i32, (128, 128), 0)
    by_domain = jnp.zeros((128, 128), f32)
    for q in range(4):
        same = domain == label_ref[q : q + 1, :]
        by_domain = by_domain + jnp.where(same, loss[q : q + 1, :], 0.0)
    column = jnp.sum(by_domain, axis=1, keepdims=True)
    eye = domain == lax.broadcasted_iota(i32, (128, 128), 1)
    line = jnp.sum(jnp.where(eye, column, 0.0), axis=0, keepdims=True)
    for t in range(8):
        sums_ref[t] = jnp.broadcast_to(line, (8, 128))


def output_kernel(sums_ref, tally, prev, old, new_ref, probs_ref):
    sums = sums_ref[0]
    for t in range(1, 8):
        sums = sums + sums_ref[t]
    sums = sums[0:1]
    reward = sums / jnp.maximum(tally[...], 1.0) / prev[...]
    new = memory_rate * old[...] + (1.0 - memory_rate) * reward
    real = lax.broadcasted_iota(i32, (1, 128), 1) < DOMAINS
    scaled = jnp.where(real, step_rate * new, -jnp.inf)
    e = jnp.exp(scaled - jnp.max(scaled, axis=1, keepdims=True))
    soft = e / jnp.sum(e, axis=1, keepdims=True)
    new_ref[...] = new[:, :DOMAINS]
    probs_ref[...] = ((1.0 - DOMAINS * explore_mass) * soft + explore_mass)[:, :DOMAINS]


def program(
    embedded, targets, labels, counts, destinations, gain_in, w_query, w_key, w_value, w_out,
    gain_out, w_vocab, prev_probs, log_weights,
):
    z, y, x, c = (lax.axis_index(a) for a in ALL)
    d, m = z * NY + y, x * NC + c
    at = jnp.stack([x, c, z, y]).astype(i32)

    w_other = shift(w_vocab, "c", 1)
    rows = w_vocab[:FRONT]
    front_1, front_3 = shift(rows, "x", 1), shift(rows, "x", 3)

    packed = call(
        pack_kernel, sds((32, 5, 8, 128), bf16),
        (embedded, targets, labels.reshape(1, 4), destinations.reshape(1, 4)),
        scratch=[pltpu.VMEM((8, 128), f32)],
    )
    got = lax.all_to_all(packed, DP, 0, 0, tiled=True)

    meta = got[:, 4]
    label_of = meta[:, 4, 0:4].reshape(128).astype(i32)
    goes_to = meta[:, 5, 0:4].reshape(128).astype(i32)
    slot = jnp.arange(128, dtype=i32)
    live = slot % 4 < jnp.repeat(counts, 4)
    chosen = live[None, :] & (goes_to[None, :] == jnp.arange(64, dtype=i32)[:, None])
    source_row = jnp.sum(jnp.where(chosen, (slot // 4) * 5 + slot % 4, 0), axis=1)
    picked = call(select_kernel, sds((64, 8, 128), bf16), (got.reshape(160, 8, 128),), source_row)
    block = lax.all_to_all(picked.reshape(32, 16, 128), DP, 0, 0, tiled=True)

    same = lax.all_gather(block, "x", axis=0, tiled=False)
    other = shift(same, "c", 1)

    cosine, sine = rope_tables()
    keep, send, resid = call(
        attention_kernel,
        [sds((4, 8, 16, 512), bf16), sds((4, 8, 16, 512), bf16), sds((8, 16, 512), bf16)],
        (
            same, other, gain_in.reshape(8, 1, 512), w_query, w_key, w_value, w_out,
            jnp.asarray(cosine), jnp.asarray(sine),
        ),
        at,
        scratch=[pltpu.VMEM((8, 16, 256), bf16)],
        flops=1 << 30,
    )
    got_part = shift(send, "c", 1)
    pair = call(pair_kernel, sds((4, 8, 16, 512), bf16), (keep, got_part))
    sums = lax.all_to_all(pair, "x", 0, 0, tiled=True)

    rows = w_vocab[FRONT:]
    late_1, late_3 = shift(rows, "x", 1), shift(rows, "x", 3)
    front_2 = shift(front_1, "x", 1)
    late_2 = shift(late_3, "x", 3)
    core_front_1, core_front_3 = shift(front_1, "c", 1), shift(front_3, "c", 1)
    core_late_1, core_late_3 = shift(late_1, "c", 1), shift(late_3, "c", 1)
    core_front_2, core_late_2 = shift(front_2, "c", 1), shift(late_2, "c", 1)

    seq_ids = jnp.dot(
        chosen.astype(bf16), meta[:, :4].reshape(128, 128), preferred_element_type=f32
    ).astype(i32)
    seq_goals = seq_ids[:, :64] * 256 + seq_ids[:, 64:]
    seq_labels = jnp.sum(jnp.where(chosen, label_of[None, :], 0), axis=1)
    mine = lax.dynamic_slice(
        seq_goals.reshape(32, 2, 4, 16), (0, m // 4, m % 4, 0), (32, 1, 1, 16)
    ).reshape(512)
    kinds = lax.dynamic_slice(seq_labels.reshape(32, 2), (0, m // 4), (32, 1))
    kinds = jnp.broadcast_to(kinds, (32, 16)).reshape(4, 128)
    goals = (mine - d * 2048).astype(f32).reshape(4, 128)
    domain = jnp.arange(128, dtype=i32)
    tally = SEQ_LEN * jnp.sum(
        (live[:, None] & (label_of[:, None] == domain[None, :])).astype(f32), axis=0
    )
    sums, goals = lax.optimization_barrier((sums, goals))

    fa, fb = call(
        final_kernel, [sds((4, 16, 512), bf16), sds((8, 4, 16, 512), bf16)],
        (resid, sums, gain_out.reshape(8, 1, 512)), at,
        scratch=[pltpu.VMEM((8, 16, 512), f32)],
    )

    parts = [shift(fa, "y", s) for s in (1, 2, 3)]
    column = lax.all_to_all(fb, "z", 0, 0, tiled=True)
    group = jnp.stack([fa, *parts])
    up, down = [group], [group]
    for _ in range(3):
        up.append(shift(up[-1], "z", 1))
        down.append(shift(down[-1], "z", NZ - 1))
    rows_b = [column] + [shift(column, "y", s) for s in (1, 2, 3)]
    up.append(shift(up[-1], "z", 1))
    rows_a = [*up, down[3], down[2], down[1]]
    weights = (
        w_vocab, front_1, late_1, front_2, late_2, front_3, late_3,
        w_other, core_front_1, core_late_1, core_front_2, core_late_2, core_front_3, core_late_3,
    )
    pieces = logits_call(at, weights, (*rows_a, *rows_b), goals)
    merged = lax.all_to_all(pieces, DP, 0, 0, tiled=True)
    losses, sums_here = call(
        merge_kernel, [sds((4, 128), f32), sds((8, 8, 128), f32)], (merged, kinds)
    )
    own_loss = lax.dynamic_slice_in_dim(losses.reshape(512), d * 16, 16, 0)
    all_sums = lax.all_to_all(sums_here, MP, 0, 0, tiled=True)
    line = lambda v, fill: jnp.pad(v, (0, 128 - DOMAINS), constant_values=fill).reshape(1, 128)
    new_weights, probs = call(
        output_kernel, [sds((1, DOMAINS), f32)] * 2,
        (all_sums, tally.reshape(1, 128), line(prev_probs, 1.0), line(log_weights, 0.0)),
    )
    return own_loss, new_weights.reshape(DOMAINS), probs.reshape(DOMAINS)


def solution(mesh):
    torus = Mesh(mesh.devices.reshape(NZ, NY, NX, NC), ALL)
    in_specs = (
        P(DP, None, MP), P(DP, None), P(DP), P(), P(DP), P(), P(None, MP), P(None, MP),
        P(None, MP), P(MP, None), P(), P(MP, DP), P(), P(),
    )
    return jax.shard_map(
        program, mesh=torus, in_specs=in_specs, out_specs=(P(ALL), P(), P()), check_vma=False
    )
```

```python
import functools

import jax
import jax.numpy as jnp
import numpy as np
from jax import lax
from jax.experimental import pallas as pl
from jax.experimental.pallas import tpu as pltpu
from jax.sharding import Mesh
from jax.sharding import PartitionSpec as P


HEAD_DIM = 128
DOMAINS = 22
SEQ_LEN = 64
DP = ("z", "y")
MP = ("x", "c")
ALL = ("z", "y", "x", "c")
NZ, NY, NX, NC = 8, 4, 4, 2

norm_eps = 1e-05
rope_base = 500000.0
memory_rate = 0.9
step_rate = 0.02
explore_mass = 0.005


bf16 = jnp.bfloat16
f32 = jnp.float32
i32 = jnp.int32


def shift(array, axis, by):
    n = {"z": NZ, "y": NY, "x": NX, "c": NC}[axis]
    return lax.ppermute(array, axis, [(i, (i + by) % n) for i in range(n)])


def call(kernel, out_shape, args, scalars=None, scratch=(), flops=0, vmem=4):
    spec = pl.BlockSpec(memory_space=pltpu.VMEM)
    many = isinstance(out_shape, (list, tuple))
    return pl.pallas_call(
        kernel,
        out_shape=out_shape,
        in_specs=([pl.BlockSpec(memory_space=pltpu.SMEM)] if scalars is not None else [])
        + [spec] * len(args),
        out_specs=[spec] * len(out_shape) if many else spec,
        scratch_shapes=scratch,
        compiler_params=pltpu.CompilerParams(vmem_limit_bytes=vmem << 20),
        cost_estimate=pl.CostEstimate(flops=flops, bytes_accessed=0, transcendentals=0)
        if flops
        else None,
    )(*(() if scalars is None else (scalars,)), *args)


def sds(shape, dtype):
    return jax.ShapeDtypeStruct(shape, dtype)


def pack_kernel(embedded, targets, labels, destinations, out_ref, meta_ref):
    ids = targets[...]
    meta_ref[...] = jnp.zeros((8, 128), f32)
    meta_ref[0:4, 0:64] = (ids // 256).astype(f32)
    meta_ref[0:4, 64:128] = (ids % 256).astype(f32)
    meta_ref[4:5, 0:4] = labels[...].astype(f32)
    meta_ref[5:6, 0:4] = destinations[...].astype(f32)
    meta = meta_ref[...].astype(bf16)
    for r in range(8):
        for col in range(4):
            for s in range(4):
                out_ref[r * 4 + col, s] = embedded[
                    s, r * 8 : r * 8 + 8, col * 128 : col * 128 + 128
                ]
            out_ref[r * 4 + col, 4] = meta


def select_kernel(row_ref, got_ref, out_ref):
    for g in range(64):
        out_ref[g] = got_ref[row_ref[g]]


def rope_tables():
    half = HEAD_DIM // 2
    frequency = np.power(rope_base, -np.arange(half) * 2.0 / HEAD_DIM)
    angle = np.arange(SEQ_LEN)[:, None] * frequency[None, :]
    cosine = np.concatenate([np.cos(angle), np.cos(angle)], axis=1)
    sine = np.concatenate([-np.sin(angle), np.sin(angle)], axis=1)
    both = [np.concatenate([t, t], axis=0).astype(np.float32) for t in (cosine, sine)]
    return both


def attention_kernel(
    at_ref, same, other, gain, wq, wk, wv, wo, cos, sin, keep_ref, send_ref, resid_ref, mixed_ref
):
    x, c = at_ref[0], at_ref[1]
    m = x * 2 + c
    blocks = [same.at[t] for t in range(4)] + [other.at[t] for t in range(4)]

    def feature_block(k):
        return (k % 4) * 2 + (c if k < 4 else 1 - c)

    def piece(ref, col):
        return jnp.concatenate([ref[r * 4 + col] for r in range(8)], axis=0).astype(f32)

    squares = jnp.zeros((128, 128), f32)
    for ref in blocks:
        for col in range(4):
            v = piece(ref, col)
            squares = squares + v * v
    inv_rms = lax.rsqrt(jnp.sum(squares, axis=1, keepdims=True) * (1.0 / 4096.0) + norm_eps)

    query = jnp.zeros((128, 256), f32)
    key = jnp.zeros((128, 128), f32)
    value = jnp.zeros((128, 128), f32)
    for k, ref in enumerate(blocks):
        fb = feature_block(k)
        g = gain[fb]
        normed = jnp.concatenate(
            [
                (piece(ref, col) * inv_rms * g[:, col * 128 : col * 128 + 128]).astype(bf16)
                for col in range(4)
            ],
            axis=1,
        )
        rows = pl.ds(pl.multiple_of(fb * 512, 512), 512)
        query = query + jnp.dot(normed, wq[rows, :], preferred_element_type=f32)
        key = key + jnp.dot(normed, wk[rows, :], preferred_element_type=f32)
        value = value + jnp.dot(normed, wv[rows, :], preferred_element_type=f32)

    def in_order(t):
        return jnp.concatenate(
            [t[r * 16 + s * 8 : r * 16 + s * 8 + 8] for s in range(2) for r in range(8)], axis=0
        )

    cosine, sine = cos[...], sin[...]

    def rotated(t):
        return (t * cosine + pltpu.roll(t, 64, axis=1) * sine).astype(bf16)

    query, key, value = in_order(query), rotated(in_order(key)), in_order(value).astype(bf16)
    row = lax.broadcasted_iota(i32, (128, 128), 0)
    column = lax.broadcasted_iota(i32, (128, 128), 1)
    seen = (row // SEQ_LEN == column // SEQ_LEN) & (column <= row)
    for h in range(2):
        q = rotated(query[:, h * 128 : h * 128 + 128])
        scores = lax.dot_general(q, key, (((1,), (1,)), ((), ())), preferred_element_type=f32)
        scores = jnp.where(seen, scores * HEAD_DIM ** (-0.5), -jnp.inf)
        top = jnp.max(scores, axis=1, keepdims=True)
        e = jnp.exp(scores - top)
        weights = (e / jnp.sum(e, axis=1, keepdims=True)).astype(bf16)
        mixed = jnp.dot(weights, value, preferred_element_type=f32).astype(bf16)
        mixed_ref[:, :, h * 128 : h * 128 + 128] = mixed.reshape(8, 16, 128)
    left = jnp.concatenate(
        [mixed_ref[t * 2 + c] for t in range(4)] + [mixed_ref[t * 2 + 1 - c] for t in range(4)],
        axis=0,
    )
    for fb in range(8):
        part = jnp.dot(left, wo[:, fb * 512 : fb * 512 + 512], preferred_element_type=f32)
        part = part.astype(bf16).reshape(8, 16, 512)
        keep_ref[:, fb] = part[:4]
        send_ref[:, fb] = part[4:]

    first = m < 4
    r0 = lax.rem(m, 4) * 2
    for k, ref in enumerate(blocks):
        fb = feature_block(k)
        rows = []
        for r in range(2):
            cols = []
            for col in range(4):
                v = ref[(r0 + r) * 4 + col].astype(f32)
                cols.append(jnp.where(first, v[:8], v[8:]))
            rows.append(jnp.concatenate(cols, axis=1))
        resid_ref[fb] = jnp.concatenate(rows, axis=0).astype(bf16)


def pair_kernel(keep_ref, got_ref, out_ref):
    out_ref[...] = (keep_ref[...].astype(f32) + got_ref[...].astype(f32)).astype(bf16)


def final_kernel(at_ref, resid, sums, gain, fa_ref, fb_ref, hidden_ref):
    x, c = at_ref[0], at_ref[1]
    squares = jnp.zeros((16, 512), f32)
    for k in range(8):
        h = resid[k].astype(f32) + (
            (sums[0, k].astype(f32) + sums[1, k].astype(f32))
            + (sums[2, k].astype(f32) + sums[3, k].astype(f32))
        )
        hidden_ref[k] = h
        squares = squares + h * h
    inv_rms = lax.rsqrt(jnp.sum(squares, axis=1, keepdims=True) * (1.0 / 4096.0) + norm_eps)
    for s in range(4):
        base = lax.rem(x + (4 - s), 4) * 2
        fa_ref[s] = (hidden_ref[base + c] * inv_rms * gain[base + c]).astype(bf16)
        other = base + 1 - c
        rows = (hidden_ref[other] * inv_rms * gain[other]).astype(bf16)
        for t in range(8):
            fb_ref[t, s] = rows


BLOCKS = 4
WIDTH = 512


FRONT = 256


def logits_kernel(at_ref, *refs):
    pieces, rows, goal_ref = refs[:14], refs[14:26], refs[26]
    (out_ref, buffer, stage_ref, rows_ref, logit_ref, top_ref, sum_ref, pick_ref, goals_ref,
     sems, row_sems) = refs[27:]
    whole, starts, at = (0, 7), [], 0
    for p in range(14):
        starts.append(at)
        at += 512 if p in whole else 256

    def copies(j):
        column = pl.ds(pl.multiple_of(j * WIDTH, WIDTH), WIDTH)
        return [
            pltpu.make_async_copy(
                ref.at[:, column],
                buffer.at[j, pl.ds(starts[p], 512 if p in whole else 256)],
                sems.at[j, p],
            )
            for p, ref in enumerate(pieces)
        ]

    row_copies = [
        pltpu.make_async_copy(ref, stage_ref.at[pl.ds(k * 256, 256)], row_sems.at[k])
        for k, ref in enumerate(rows[:8])
    ] + [
        pltpu.make_async_copy(ref, stage_ref.at[pl.ds(2048 + k * 512, 512)], row_sems.at[8 + k])
        for k, ref in enumerate(rows[8:])
    ]
    for copy in row_copies:
        copy.start()

    @pl.loop(0, BLOCKS)
    def _(j):
        for copy in copies(j):
            copy.start()

    eye = lax.broadcasted_iota(i32, (128, 128), 0) == lax.broadcasted_iota(i32, (128, 128), 1)
    for q in range(4):
        goals_ref[q * 128 : q * 128 + 128] = jnp.sum(
            jnp.where(eye, goal_ref[q : q + 1], 0.0), axis=1, keepdims=True
        )
    top_ref[...] = jnp.full((512, 1), -jnp.inf, f32)
    sum_ref[...] = jnp.zeros((512, 1), f32)
    pick_ref[...] = jnp.zeros((512, 1), f32)

    for copy in row_copies:
        copy.wait()
    z, y = at_ref[2], at_ref[3]
    for dz in range(8):
        for dy in range(4):
            in_y = lax.rem(y + (4 - dy), 4)
            a_rows = pl.ds(pl.multiple_of((lax.rem(z + (8 - dz), 8) * 4 + in_y) * 16, 16), 16)
            b_rows = pl.ds(pl.multiple_of((dz * 4 + in_y) * 16, 16), 16)
            for k in range(4):
                lo = dz * 256 + (dy * 4 + k) * 16
                rows_ref[a_rows, k * 512 : k * 512 + 512] = stage_ref[lo : lo + 16]
                lo = 2048 + dy * 512 + (dz * 4 + k) * 16
                rows_ref[b_rows, 2048 + k * 512 : 2560 + k * 512] = stage_ref[lo : lo + 16]

    def multiply(j):
        for copy in copies(j):
            copy.wait()
        return jnp.dot(rows_ref[...], buffer[j], preferred_element_type=f32)

    def reduce(j, logits):
        column = lax.broadcasted_iota(i32, logits.shape, 1).astype(f32)
        top = top_ref[...]
        new = jnp.maximum(top, jnp.max(logits, axis=1, keepdims=True))
        sum_ref[...] = sum_ref[...] * jnp.exp(top - new) + jnp.sum(
            jnp.exp(logits - new), axis=1, keepdims=True
        )
        hit = column == goals_ref[...] - lax.convert_element_type(j * WIDTH, f32)
        pick_ref[...] += jnp.sum(jnp.where(hit, logits, 0.0), axis=1, keepdims=True)
        top_ref[...] = new

    logit_ref[0] = multiply(0)

    @pl.loop(1, BLOCKS)
    def _(j):
        logits = multiply(j)
        reduce(j - 1, logit_ref[lax.rem(j - 1, 2)])
        logit_ref[lax.rem(j, 2)] = logits

    reduce(jnp.int32(BLOCKS - 1), logit_ref[(BLOCKS - 1) % 2])
    lines = []
    for values in (top_ref[...] + jnp.log(sum_ref[...]), pick_ref[...]):
        for q in range(4):
            block = jnp.where(eye, values[q * 128 : q * 128 + 128], 0.0)
            lines.append(jnp.sum(block, axis=0, keepdims=True))
    lines = jnp.concatenate(lines, axis=0)
    for t in range(32):
        out_ref[t] = lines


def logits_call(at, weights, rows, goals):
    vmem = pl.BlockSpec(memory_space=pltpu.VMEM)
    hbm = pl.BlockSpec(memory_space=pltpu.HBM)
    rows = [r.reshape(-1, 512) for r in rows]
    return pl.pallas_call(
        logits_kernel,
        out_shape=sds((32, 8, 128), f32),
        in_specs=[pl.BlockSpec(memory_space=pltpu.SMEM)]
        + [hbm] * (len(weights) + len(rows))
        + [vmem],
        out_specs=vmem,
        scratch_shapes=[
            pltpu.VMEM((BLOCKS, 4096, WIDTH), bf16),
            pltpu.VMEM((4096, 512), bf16),
            pltpu.VMEM((512, 4096), bf16),
            pltpu.VMEM((2, 512, WIDTH), f32),
            pltpu.VMEM((512, 1), f32),
            pltpu.VMEM((512, 1), f32),
            pltpu.VMEM((512, 1), f32),
            pltpu.VMEM((512, 1), f32),
            pltpu.SemaphoreType.DMA((BLOCKS, 14)),
            pltpu.SemaphoreType.DMA((12,)),
        ],
        name="logits",
        cost_estimate=pl.CostEstimate(
            flops=2 * 512 * 4096 * 2048, bytes_accessed=20 << 20, transcendentals=0
        ),
        compiler_params=pltpu.CompilerParams(vmem_limit_bytes=36 << 20),
    )(at, *weights, *rows, goals)


def merge_kernel(got_ref, label_ref, loss_ref, sums_ref):
    lse = [got_ref[k][:4] for k in range(32)]
    top = functools.reduce(jnp.maximum, lse)
    total = functools.reduce(lambda a, b: a + b, [jnp.exp(v - top) for v in lse])
    picked = functools.reduce(lambda a, b: a + b, [got_ref[k][4:] for k in range(32)])
    loss = top + jnp.log(total) - picked
    loss_ref[...] = loss
    domain = lax.broadcasted_iota(i32, (128, 128), 0)
    by_domain = jnp.zeros((128, 128), f32)
    for q in range(4):
        same = domain == label_ref[q : q + 1, :]
        by_domain = by_domain + jnp.where(same, loss[q : q + 1, :], 0.0)
    column = jnp.sum(by_domain, axis=1, keepdims=True)
    eye = domain == lax.broadcasted_iota(i32, (128, 128), 1)
    line = jnp.sum(jnp.where(eye, column, 0.0), axis=0, keepdims=True)
    for t in range(8):
        sums_ref[t] = jnp.broadcast_to(line, (8, 128))


def output_kernel(sums_ref, tally, prev, old, new_ref, probs_ref):
    sums = sums_ref[0]
    for t in range(1, 8):
        sums = sums + sums_ref[t]
    sums = sums[0:1]
    reward = sums / jnp.maximum(tally[...], 1.0) / prev[...]
    new = memory_rate * old[...] + (1.0 - memory_rate) * reward
    real = lax.broadcasted_iota(i32, (1, 128), 1) < DOMAINS
    scaled = jnp.where(real, step_rate * new, -jnp.inf)
    e = jnp.exp(scaled - jnp.max(scaled, axis=1, keepdims=True))
    soft = e / jnp.sum(e, axis=1, keepdims=True)
    new_ref[...] = new[:, :DOMAINS]
    probs_ref[...] = ((1.0 - DOMAINS * explore_mass) * soft + explore_mass)[:, :DOMAINS]


def program(
    embedded, targets, labels, counts, destinations, gain_in, w_query, w_key, w_value, w_out,
    gain_out, w_vocab, prev_probs, log_weights,
):
    z, y, x, c = (lax.axis_index(a) for a in ALL)
    d, m = z * NY + y, x * NC + c
    at = jnp.stack([x, c, z, y]).astype(i32)

    w_other = shift(w_vocab, "c", 1)
    rows = w_vocab[:FRONT]
    front_1, front_3 = shift(rows, "x", 1), shift(rows, "x", 3)

    packed = call(
        pack_kernel, sds((32, 5, 8, 128), bf16),
        (embedded, targets, labels.reshape(1, 4), destinations.reshape(1, 4)),
        scratch=[pltpu.VMEM((8, 128), f32)], vmem=60,
    )
    got = lax.all_to_all(packed, DP, 0, 0, tiled=True)

    meta = got[:, 4]
    label_of = meta[:, 4, 0:4].reshape(128).astype(i32)
    goes_to = meta[:, 5, 0:4].reshape(128).astype(i32)
    slot = jnp.arange(128, dtype=i32)
    live = slot % 4 < jnp.repeat(counts, 4)
    chosen = live[None, :] & (goes_to[None, :] == jnp.arange(64, dtype=i32)[:, None])
    source_row = jnp.sum(jnp.where(chosen, (slot // 4) * 5 + slot % 4, 0), axis=1)
    picked = call(select_kernel, sds((64, 8, 128), bf16), (got.reshape(160, 8, 128),), source_row)
    block = lax.all_to_all(picked.reshape(32, 16, 128), DP, 0, 0, tiled=True)

    same = lax.all_gather(block, "x", axis=0, tiled=False)
    other = shift(same, "c", 1)

    cosine, sine = rope_tables()
    keep, send, resid = call(
        attention_kernel,
        [sds((4, 8, 16, 512), bf16), sds((4, 8, 16, 512), bf16), sds((8, 16, 512), bf16)],
        (
            same, other, gain_in.reshape(8, 1, 512), w_query, w_key, w_value, w_out,
            jnp.asarray(cosine), jnp.asarray(sine),
        ),
        at,
        scratch=[pltpu.VMEM((8, 16, 256), bf16)],
        flops=1 << 30,
        vmem=60,
    )
    got_part = shift(send, "c", 1)
    pair = call(pair_kernel, sds((4, 8, 16, 512), bf16), (keep, got_part))
    sums = lax.all_to_all(pair, "x", 0, 0, tiled=True)

    rows = w_vocab[FRONT:]
    late_1, late_3 = shift(rows, "x", 1), shift(rows, "x", 3)
    front_2 = shift(front_1, "x", 1)
    late_2 = shift(late_3, "x", 3)
    core_front_1, core_front_3 = shift(front_1, "c", 1), shift(front_3, "c", 1)
    core_late_1, core_late_3 = shift(late_1, "c", 1), shift(late_3, "c", 1)
    core_front_2, core_late_2 = shift(front_2, "c", 1), shift(late_2, "c", 1)

    seq_ids = jnp.dot(
        chosen.astype(bf16), meta[:, :4].reshape(128, 128), preferred_element_type=f32
    ).astype(i32)
    seq_goals = seq_ids[:, :64] * 256 + seq_ids[:, 64:]
    seq_labels = jnp.sum(jnp.where(chosen, label_of[None, :], 0), axis=1)
    mine = lax.dynamic_slice(
        seq_goals.reshape(32, 2, 4, 16), (0, m // 4, m % 4, 0), (32, 1, 1, 16)
    ).reshape(512)
    kinds = lax.dynamic_slice(seq_labels.reshape(32, 2), (0, m // 4), (32, 1))
    kinds = jnp.broadcast_to(kinds, (32, 16)).reshape(4, 128)
    goals = (mine - d * 2048).astype(f32).reshape(4, 128)
    domain = jnp.arange(128, dtype=i32)
    tally = SEQ_LEN * jnp.sum(
        (live[:, None] & (label_of[:, None] == domain[None, :])).astype(f32), axis=0
    )
    sums, goals = lax.optimization_barrier((sums, goals))

    fa, fb = call(
        final_kernel, [sds((4, 16, 512), bf16), sds((8, 4, 16, 512), bf16)],
        (resid, sums, gain_out.reshape(8, 1, 512)), at,
        scratch=[pltpu.VMEM((8, 16, 512), f32)],
    )

    parts = [shift(fa, "y", s) for s in (1, 2, 3)]
    column = lax.all_to_all(fb, "z", 0, 0, tiled=True)
    group = jnp.stack([fa, *parts])
    up, down = [group], [group]
    for _ in range(3):
        up.append(shift(up[-1], "z", 1))
        down.append(shift(down[-1], "z", NZ - 1))
    rows_b = [column] + [shift(column, "y", s) for s in (1, 2, 3)]
    up.append(shift(up[-1], "z", 1))
    rows_a = [*up, down[3], down[2], down[1]]
    weights = (
        w_vocab, front_1, late_1, front_2, late_2, front_3, late_3,
        w_other, core_front_1, core_late_1, core_front_2, core_late_2, core_front_3, core_late_3,
    )
    pieces = logits_call(at, weights, (*rows_a, *rows_b), goals)
    merged = lax.all_to_all(pieces, DP, 0, 0, tiled=True)
    losses, sums_here = call(
        merge_kernel, [sds((4, 128), f32), sds((8, 8, 128), f32)], (merged, kinds)
    )
    own_loss = lax.dynamic_slice_in_dim(losses.reshape(512), d * 16, 16, 0)
    all_sums = lax.all_to_all(sums_here, MP, 0, 0, tiled=True)
    line = lambda v, fill: jnp.pad(v, (0, 128 - DOMAINS), constant_values=fill).reshape(1, 128)
    new_weights, probs = call(
        output_kernel, [sds((1, DOMAINS), f32)] * 2,
        (all_sums, tally.reshape(1, 128), line(prev_probs, 1.0), line(log_weights, 0.0)),
    )
    return own_loss, new_weights.reshape(DOMAINS), probs.reshape(DOMAINS)


def solution(mesh):
    torus = Mesh(mesh.devices.reshape(NZ, NY, NX, NC), ALL)
    in_specs = (
        P(DP, None, MP), P(DP, None), P(DP), P(), P(DP), P(), P(None, MP), P(None, MP),
        P(None, MP), P(MP, None), P(), P(MP, DP), P(), P(),
    )
    return jax.shard_map(
        program, mesh=torus, in_specs=in_specs, out_specs=(P(ALL), P(), P()), check_vma=False
    )
```

```python
import functools

import jax
import jax.numpy as jnp
import numpy as np
from jax import lax
from jax.experimental import pallas as pl
from jax.experimental.pallas import tpu as pltpu
from jax.sharding import Mesh
from jax.sharding import PartitionSpec as P


HEAD_DIM = 128
DOMAINS = 22
SEQ_LEN = 64
DP = ("z", "y")
MP = ("x", "c")
ALL = ("z", "y", "x", "c")
NZ, NY, NX, NC = 8, 4, 4, 2

norm_eps = 1e-05
rope_base = 500000.0
memory_rate = 0.9
step_rate = 0.02
explore_mass = 0.005


bf16 = jnp.bfloat16
f32 = jnp.float32
i32 = jnp.int32


def shift(array, axis, by):
    n = {"z": NZ, "y": NY, "x": NX, "c": NC}[axis]
    return lax.ppermute(array, axis, [(i, (i + by) % n) for i in range(n)])


def call(kernel, out_shape, args, scalars=None, scratch=(), flops=0, vmem=4):
    spec = pl.BlockSpec(memory_space=pltpu.VMEM)
    many = isinstance(out_shape, (list, tuple))
    return pl.pallas_call(
        kernel,
        out_shape=out_shape,
        in_specs=([pl.BlockSpec(memory_space=pltpu.SMEM)] if scalars is not None else [])
        + [spec] * len(args),
        out_specs=[spec] * len(out_shape) if many else spec,
        scratch_shapes=scratch,
        compiler_params=pltpu.CompilerParams(vmem_limit_bytes=vmem << 20),
        cost_estimate=pl.CostEstimate(flops=flops, bytes_accessed=0, transcendentals=0)
        if flops
        else None,
    )(*(() if scalars is None else (scalars,)), *args)


def sds(shape, dtype):
    return jax.ShapeDtypeStruct(shape, dtype)


def pack_kernel(embedded, targets, labels, destinations, out_ref, meta_ref):
    ids = targets[...]
    meta_ref[...] = jnp.zeros((8, 128), f32)
    meta_ref[0:4, 0:64] = (ids // 256).astype(f32)
    meta_ref[0:4, 64:128] = (ids % 256).astype(f32)
    meta_ref[4:5, 0:4] = labels[...].astype(f32)
    meta_ref[5:6, 0:4] = destinations[...].astype(f32)
    meta = meta_ref[...].astype(bf16)
    for r in range(8):
        for col in range(4):
            for s in range(4):
                out_ref[r * 4 + col, s] = embedded[
                    s, r * 8 : r * 8 + 8, col * 128 : col * 128 + 128
                ]
            out_ref[r * 4 + col, 4] = meta


def select_kernel(row_ref, got_ref, out_ref):
    for g in range(64):
        out_ref[g] = got_ref[row_ref[g]]


def rope_tables():
    half = HEAD_DIM // 2
    frequency = np.power(rope_base, -np.arange(half) * 2.0 / HEAD_DIM)
    angle = np.arange(SEQ_LEN)[:, None] * frequency[None, :]
    cosine = np.concatenate([np.cos(angle), np.cos(angle)], axis=1)
    sine = np.concatenate([-np.sin(angle), np.sin(angle)], axis=1)
    both = [np.concatenate([t, t], axis=0).astype(np.float32) for t in (cosine, sine)]
    return both


def attention_kernel(
    at_ref, same, other, gain, wq, wk, wv, wo, cos, sin, keep_ref, send_ref, resid_ref, mixed_ref
):
    x, c = at_ref[0], at_ref[1]
    m = x * 2 + c
    blocks = [same.at[t] for t in range(4)] + [other.at[t] for t in range(4)]

    def feature_block(k):
        return (k % 4) * 2 + (c if k < 4 else 1 - c)

    def piece(ref, col):
        return jnp.concatenate([ref[r * 4 + col] for r in range(8)], axis=0).astype(f32)

    squares = jnp.zeros((128, 128), f32)
    for ref in blocks:
        for col in range(4):
            v = piece(ref, col)
            squares = squares + v * v
    inv_rms = lax.rsqrt(jnp.sum(squares, axis=1, keepdims=True) * (1.0 / 4096.0) + norm_eps)

    query = jnp.zeros((128, 256), f32)
    key = jnp.zeros((128, 128), f32)
    value = jnp.zeros((128, 128), f32)
    for k, ref in enumerate(blocks):
        fb = feature_block(k)
        g = gain[fb]
        normed = jnp.concatenate(
            [
                (piece(ref, col) * inv_rms * g[:, col * 128 : col * 128 + 128]).astype(bf16)
                for col in range(4)
            ],
            axis=1,
        )
        rows = pl.ds(pl.multiple_of(fb * 512, 512), 512)
        query = query + jnp.dot(normed, wq[rows, :], preferred_element_type=f32)
        key = key + jnp.dot(normed, wk[rows, :], preferred_element_type=f32)
        value = value + jnp.dot(normed, wv[rows, :], preferred_element_type=f32)

    def in_order(t):
        return jnp.concatenate(
            [t[r * 16 + s * 8 : r * 16 + s * 8 + 8] for s in range(2) for r in range(8)], axis=0
        )

    cosine, sine = cos[...], sin[...]

    def rotated(t):
        return (t * cosine + pltpu.roll(t, 64, axis=1) * sine).astype(bf16)

    query, key, value = in_order(query), rotated(in_order(key)), in_order(value).astype(bf16)
    row = lax.broadcasted_iota(i32, (128, 128), 0)
    column = lax.broadcasted_iota(i32, (128, 128), 1)
    seen = (row // SEQ_LEN == column // SEQ_LEN) & (column <= row)
    for h in range(2):
        q = rotated(query[:, h * 128 : h * 128 + 128])
        scores = lax.dot_general(q, key, (((1,), (1,)), ((), ())), preferred_element_type=f32)
        scores = jnp.where(seen, scores * HEAD_DIM ** (-0.5), -jnp.inf)
        top = jnp.max(scores, axis=1, keepdims=True)
        e = jnp.exp(scores - top)
        weights = (e / jnp.sum(e, axis=1, keepdims=True)).astype(bf16)
        mixed = jnp.dot(weights, value, preferred_element_type=f32).astype(bf16)
        mixed_ref[:, :, h * 128 : h * 128 + 128] = mixed.reshape(8, 16, 128)
    left = jnp.concatenate(
        [mixed_ref[t * 2 + c] for t in range(4)] + [mixed_ref[t * 2 + 1 - c] for t in range(4)],
        axis=0,
    )
    for fb in range(8):
        part = jnp.dot(left, wo[:, fb * 512 : fb * 512 + 512], preferred_element_type=f32)
        part = part.astype(bf16).reshape(8, 16, 512)
        keep_ref[:, fb] = part[:4]
        send_ref[:, fb] = part[4:]

    first = m < 4
    r0 = lax.rem(m, 4) * 2
    for k, ref in enumerate(blocks):
        fb = feature_block(k)
        rows = []
        for r in range(2):
            cols = []
            for col in range(4):
                v = ref[(r0 + r) * 4 + col].astype(f32)
                cols.append(jnp.where(first, v[:8], v[8:]))
            rows.append(jnp.concatenate(cols, axis=1))
        resid_ref[fb] = jnp.concatenate(rows, axis=0).astype(bf16)


def final_kernel(at_ref, resid, sums, gain, fa_ref, fb_ref, hidden_ref):
    x, c = at_ref[0], at_ref[1]
    squares = jnp.zeros((16, 512), f32)
    for k in range(8):
        h = resid[k].astype(f32) + (
            (sums[0, k].astype(f32) + sums[1, k].astype(f32))
            + (sums[2, k].astype(f32) + sums[3, k].astype(f32))
        )
        hidden_ref[k] = h
        squares = squares + h * h
    inv_rms = lax.rsqrt(jnp.sum(squares, axis=1, keepdims=True) * (1.0 / 4096.0) + norm_eps)
    for s in range(4):
        base = lax.rem(x + (4 - s), 4) * 2
        fa_ref[s] = (hidden_ref[base + c] * inv_rms * gain[base + c]).astype(bf16)
        other = base + 1 - c
        rows = (hidden_ref[other] * inv_rms * gain[other]).astype(bf16)
        for t in range(8):
            fb_ref[t, s] = rows


BLOCKS = 4
WIDTH = 512


FRONT = 256


def logits_kernel(at_ref, *refs):
    pieces, rows_a, rows_b, goal_ref = refs[:14], refs[14:22], refs[22:26], refs[26]
    (out_ref, buffer, rows_ref, logit_ref, top_ref, sum_ref, pick_ref, goals_ref,
     sems) = refs[27:]
    whole, starts, at = (0, 7), [], 0
    for p in range(14):
        starts.append(at)
        at += 512 if p in whole else 256

    def copies(j):
        column = pl.ds(pl.multiple_of(j * WIDTH, WIDTH), WIDTH)
        return [
            pltpu.make_async_copy(
                ref.at[:, column],
                buffer.at[j, pl.ds(starts[p], 512 if p in whole else 256)],
                sems.at[j, p],
            )
            for p, ref in enumerate(pieces)
        ]

    @pl.loop(0, BLOCKS)
    def _(j):
        for copy in copies(j):
            copy.start()

    eye = lax.broadcasted_iota(i32, (128, 128), 0) == lax.broadcasted_iota(i32, (128, 128), 1)
    for q in range(4):
        goals_ref[q * 128 : q * 128 + 128] = jnp.sum(
            jnp.where(eye, goal_ref[q : q + 1], 0.0), axis=1, keepdims=True
        )
    top_ref[...] = jnp.full((512, 1), -jnp.inf, f32)
    sum_ref[...] = jnp.zeros((512, 1), f32)
    pick_ref[...] = jnp.zeros((512, 1), f32)

    z, y = at_ref[2], at_ref[3]
    for dz in range(8):
        for dy in range(4):
            in_y = lax.rem(y + (4 - dy), 4)
            a_rows = pl.ds(pl.multiple_of((lax.rem(z + (8 - dz), 8) * 4 + in_y) * 16, 16), 16)
            b_rows = pl.ds(pl.multiple_of((dz * 4 + in_y) * 16, 16), 16)
            for k in range(4):
                rows_ref[a_rows, k * 512 : k * 512 + 512] = rows_a[dz][dy, k]
                rows_ref[b_rows, 2048 + k * 512 : 2560 + k * 512] = rows_b[dy][dz, k]

    def multiply(j):
        for copy in copies(j):
            copy.wait()
        return jnp.dot(rows_ref[...], buffer[j], preferred_element_type=f32)

    def reduce(j, logits):
        column = lax.broadcasted_iota(i32, logits.shape, 1).astype(f32)
        top = top_ref[...]
        new = jnp.maximum(top, jnp.max(logits, axis=1, keepdims=True))
        sum_ref[...] = sum_ref[...] * jnp.exp(top - new) + jnp.sum(
            jnp.exp(logits - new), axis=1, keepdims=True
        )
        hit = column == goals_ref[...] - lax.convert_element_type(j * WIDTH, f32)
        pick_ref[...] += jnp.sum(jnp.where(hit, logits, 0.0), axis=1, keepdims=True)
        top_ref[...] = new

    logit_ref[0] = multiply(0)

    @pl.loop(1, BLOCKS)
    def _(j):
        logits = multiply(j)
        reduce(j - 1, logit_ref[lax.rem(j - 1, 2)])
        logit_ref[lax.rem(j, 2)] = logits

    reduce(jnp.int32(BLOCKS - 1), logit_ref[(BLOCKS - 1) % 2])
    lines = []
    for values in (top_ref[...] + jnp.log(sum_ref[...]), pick_ref[...]):
        for q in range(4):
            block = jnp.where(eye, values[q * 128 : q * 128 + 128], 0.0)
            lines.append(jnp.sum(block, axis=0, keepdims=True))
    lines = jnp.concatenate(lines, axis=0)
    for t in range(32):
        out_ref[t] = lines


def logits_call(at, weights, rows, goals):
    vmem = pl.BlockSpec(memory_space=pltpu.VMEM)
    hbm = pl.BlockSpec(memory_space=pltpu.HBM)
    return pl.pallas_call(
        logits_kernel,
        out_shape=sds((32, 8, 128), f32),
        in_specs=[pl.BlockSpec(memory_space=pltpu.SMEM)]
        + [hbm] * len(weights)
        + [vmem] * (len(rows) + 1),
        out_specs=vmem,
        scratch_shapes=[
            pltpu.VMEM((BLOCKS, 4096, WIDTH), bf16),
            pltpu.VMEM((512, 4096), bf16),
            pltpu.VMEM((2, 512, WIDTH), f32),
            pltpu.VMEM((512, 1), f32),
            pltpu.VMEM((512, 1), f32),
            pltpu.VMEM((512, 1), f32),
            pltpu.VMEM((512, 1), f32),
            pltpu.SemaphoreType.DMA((BLOCKS, 14)),
        ],
        name="logits",
        cost_estimate=pl.CostEstimate(
            flops=2 * 512 * 4096 * 2048, bytes_accessed=20 << 20, transcendentals=0
        ),
        compiler_params=pltpu.CompilerParams(vmem_limit_bytes=36 << 20),
    )(at, *weights, *rows, goals)


def merge_kernel(got_ref, label_ref, loss_ref, sums_ref):
    lse = [got_ref[k][:4] for k in range(32)]
    top = functools.reduce(jnp.maximum, lse)
    total = functools.reduce(lambda a, b: a + b, [jnp.exp(v - top) for v in lse])
    picked = functools.reduce(lambda a, b: a + b, [got_ref[k][4:] for k in range(32)])
    loss = top + jnp.log(total) - picked
    loss_ref[...] = loss
    domain = lax.broadcasted_iota(i32, (128, 128), 0)
    by_domain = jnp.zeros((128, 128), f32)
    for q in range(4):
        same = domain == label_ref[q : q + 1, :]
        by_domain = by_domain + jnp.where(same, loss[q : q + 1, :], 0.0)
    column = jnp.sum(by_domain, axis=1, keepdims=True)
    eye = domain == lax.broadcasted_iota(i32, (128, 128), 1)
    line = jnp.sum(jnp.where(eye, column, 0.0), axis=0, keepdims=True)
    for t in range(8):
        sums_ref[t] = jnp.broadcast_to(line, (8, 128))


def output_kernel(sums_ref, tally, prev, old, new_ref, probs_ref):
    sums = sums_ref[0]
    for t in range(1, 8):
        sums = sums + sums_ref[t]
    sums = sums[0:1]
    reward = sums / jnp.maximum(tally[...], 1.0) / prev[...]
    new = memory_rate * old[...] + (1.0 - memory_rate) * reward
    real = lax.broadcasted_iota(i32, (1, 128), 1) < DOMAINS
    scaled = jnp.where(real, step_rate * new, -jnp.inf)
    e = jnp.exp(scaled - jnp.max(scaled, axis=1, keepdims=True))
    soft = e / jnp.sum(e, axis=1, keepdims=True)
    new_ref[...] = new[:, :DOMAINS]
    probs_ref[...] = ((1.0 - DOMAINS * explore_mass) * soft + explore_mass)[:, :DOMAINS]


def program(
    embedded, targets, labels, counts, destinations, gain_in, w_query, w_key, w_value, w_out,
    gain_out, w_vocab, prev_probs, log_weights,
):
    z, y, x, c = (lax.axis_index(a) for a in ALL)
    d, m = z * NY + y, x * NC + c
    at = jnp.stack([x, c, z, y]).astype(i32)

    w_other = shift(w_vocab, "c", 1)
    rows = w_vocab[:FRONT]
    front_1, front_3 = shift(rows, "x", 1), shift(rows, "x", 3)

    packed = call(
        pack_kernel, sds((32, 5, 8, 128), bf16),
        (embedded, targets, labels.reshape(1, 4), destinations.reshape(1, 4)),
        scratch=[pltpu.VMEM((8, 128), f32)], vmem=60,
    )
    got = lax.all_to_all(packed, DP, 0, 0, tiled=True)

    meta = got[:, 4]
    label_of = meta[:, 4, 0:4].reshape(128).astype(i32)
    goes_to = meta[:, 5, 0:4].reshape(128).astype(i32)
    slot = jnp.arange(128, dtype=i32)
    live = slot % 4 < jnp.repeat(counts, 4)
    chosen = live[None, :] & (goes_to[None, :] == jnp.arange(64, dtype=i32)[:, None])
    source_row = jnp.sum(jnp.where(chosen, (slot // 4) * 5 + slot % 4, 0), axis=1)
    picked = call(select_kernel, sds((64, 8, 128), bf16), (got.reshape(160, 8, 128),), source_row)
    block = lax.all_to_all(picked.reshape(32, 16, 128), DP, 0, 0, tiled=True)

    same = lax.all_gather(block, "x", axis=0, tiled=False)
    other = shift(same, "c", 1)

    cosine, sine = rope_tables()
    keep, send, resid = call(
        attention_kernel,
        [sds((4, 8, 16, 512), bf16), sds((4, 8, 16, 512), bf16), sds((8, 16, 512), bf16)],
        (
            same, other, gain_in.reshape(8, 1, 512), w_query, w_key, w_value, w_out,
            jnp.asarray(cosine), jnp.asarray(sine),
        ),
        at,
        scratch=[pltpu.VMEM((8, 16, 256), bf16)],
        flops=1 << 30,
        vmem=60,
    )
    got_part = shift(send, "c", 1)
    pair = (keep.astype(f32) + got_part.astype(f32)).astype(bf16)
    sums = lax.all_to_all(pair, "x", 0, 0, tiled=True)

    rows = w_vocab[FRONT:]
    late_1, late_3 = shift(rows, "x", 1), shift(rows, "x", 3)
    front_2 = shift(front_1, "x", 1)
    late_2 = shift(late_3, "x", 3)
    core_front_1, core_front_3 = shift(front_1, "c", 1), shift(front_3, "c", 1)
    core_late_1, core_late_3 = shift(late_1, "c", 1), shift(late_3, "c", 1)
    core_front_2, core_late_2 = shift(front_2, "c", 1), shift(late_2, "c", 1)

    seq_ids = jnp.dot(
        chosen.astype(bf16), meta[:, :4].reshape(128, 128), preferred_element_type=f32
    ).astype(i32)
    seq_goals = seq_ids[:, :64] * 256 + seq_ids[:, 64:]
    seq_labels = jnp.sum(jnp.where(chosen, label_of[None, :], 0), axis=1)
    mine = lax.dynamic_slice(
        seq_goals.reshape(32, 2, 4, 16), (0, m // 4, m % 4, 0), (32, 1, 1, 16)
    ).reshape(512)
    kinds = lax.dynamic_slice(seq_labels.reshape(32, 2), (0, m // 4), (32, 1))
    kinds = jnp.broadcast_to(kinds, (32, 16)).reshape(4, 128)
    goals = (mine - d * 2048).astype(f32).reshape(4, 128)
    domain = jnp.arange(128, dtype=i32)
    tally = SEQ_LEN * jnp.sum(
        (live[:, None] & (label_of[:, None] == domain[None, :])).astype(f32), axis=0
    )
    sums, goals = lax.optimization_barrier((sums, goals))

    fa, fb = call(
        final_kernel, [sds((4, 16, 512), bf16), sds((8, 4, 16, 512), bf16)],
        (resid, sums, gain_out.reshape(8, 1, 512)), at,
        scratch=[pltpu.VMEM((8, 16, 512), f32)],
    )

    parts = [shift(fa, "y", s) for s in (1, 2, 3)]
    column = lax.all_to_all(fb, "z", 0, 0, tiled=True)
    group = jnp.stack([fa, *parts])
    up, down = [group], [group]
    for _ in range(3):
        up.append(shift(up[-1], "z", 1))
        down.append(shift(down[-1], "z", NZ - 1))
    rows_b = [column] + [shift(column, "y", s) for s in (1, 2, 3)]
    up.append(shift(up[-1], "z", 1))
    rows_a = [*up, down[3], down[2], down[1]]
    weights = (
        w_vocab, front_1, late_1, front_2, late_2, front_3, late_3,
        w_other, core_front_1, core_late_1, core_front_2, core_late_2, core_front_3, core_late_3,
    )
    pieces = logits_call(at, weights, (*rows_a, *rows_b), goals)
    merged = lax.all_to_all(pieces, DP, 0, 0, tiled=True)
    losses, sums_here = call(
        merge_kernel, [sds((4, 128), f32), sds((8, 8, 128), f32)], (merged, kinds)
    )
    own_loss = lax.dynamic_slice_in_dim(losses.reshape(512), d * 16, 16, 0)
    all_sums = lax.all_to_all(sums_here, MP, 0, 0, tiled=True)
    line = lambda v, fill: jnp.pad(v, (0, 128 - DOMAINS), constant_values=fill).reshape(1, 128)
    new_weights, probs = call(
        output_kernel, [sds((1, DOMAINS), f32)] * 2,
        (all_sums, tally.reshape(1, 128), line(prev_probs, 1.0), line(log_weights, 0.0)),
    )
    return own_loss, new_weights.reshape(DOMAINS), probs.reshape(DOMAINS)


def solution(mesh):
    torus = Mesh(mesh.devices.reshape(NZ, NY, NX, NC), ALL)
    in_specs = (
        P(DP, None, MP), P(DP, None), P(DP), P(), P(DP), P(), P(None, MP), P(None, MP),
        P(None, MP), P(MP, None), P(), P(MP, DP), P(), P(),
    )
    return jax.shard_map(
        program, mesh=torus, in_specs=in_specs, out_specs=(P(ALL), P(), P()), check_vma=False
    )
```

```python
import functools

import jax
import jax.numpy as jnp
import numpy as np
from jax import lax
from jax.experimental import pallas as pl
from jax.experimental.pallas import tpu as pltpu
from jax.sharding import Mesh
from jax.sharding import PartitionSpec as P


HEAD_DIM = 128
DOMAINS = 22
SEQ_LEN = 64
DP = ("z", "y")
MP = ("x", "c")
ALL = ("z", "y", "x", "c")
NZ, NY, NX, NC = 8, 4, 4, 2

norm_eps = 1e-05
rope_base = 500000.0
memory_rate = 0.9
step_rate = 0.02
explore_mass = 0.005


bf16 = jnp.bfloat16
f32 = jnp.float32
i32 = jnp.int32


def shift(array, axis, by):
    n = {"z": NZ, "y": NY, "x": NX, "c": NC}[axis]
    return lax.ppermute(array, axis, [(i, (i + by) % n) for i in range(n)])


def call(kernel, out_shape, args, scalars=None, scratch=(), flops=0, vmem=4, far=0):
    spec = pl.BlockSpec(memory_space=pltpu.VMEM)
    many = isinstance(out_shape, (list, tuple))
    return pl.pallas_call(
        kernel,
        out_shape=out_shape,
        in_specs=([pl.BlockSpec(memory_space=pltpu.SMEM)] if scalars is not None else [])
        + [spec] * (len(args) - far)
        + [pl.BlockSpec(memory_space=pltpu.HBM)] * far,
        out_specs=[spec] * len(out_shape) if many else spec,
        scratch_shapes=scratch,
        compiler_params=pltpu.CompilerParams(vmem_limit_bytes=vmem << 20),
        cost_estimate=pl.CostEstimate(flops=flops, bytes_accessed=0, transcendentals=0)
        if flops
        else None,
    )(*(() if scalars is None else (scalars,)), *args)


def sds(shape, dtype):
    return jax.ShapeDtypeStruct(shape, dtype)


def pack_kernel(embedded, targets, labels, destinations, out_ref, meta_ref):
    ids = targets[...]
    meta_ref[...] = jnp.zeros((8, 128), f32)
    meta_ref[0:4, 0:64] = (ids // 256).astype(f32)
    meta_ref[0:4, 64:128] = (ids % 256).astype(f32)
    meta_ref[4:5, 0:4] = labels[...].astype(f32)
    meta_ref[5:6, 0:4] = destinations[...].astype(f32)
    meta = meta_ref[...].astype(bf16)
    for r in range(8):
        for col in range(4):
            for s in range(4):
                out_ref[r * 4 + col, s] = embedded[
                    s, r * 8 : r * 8 + 8, col * 128 : col * 128 + 128
                ]
            out_ref[r * 4 + col, 4] = meta


def select_kernel(row_ref, got_ref, out_ref):
    for g in range(64):
        out_ref[g] = got_ref[row_ref[g]]


def rope_tables():
    half = HEAD_DIM // 2
    frequency = np.power(rope_base, -np.arange(half) * 2.0 / HEAD_DIM)
    angle = np.arange(SEQ_LEN)[:, None] * frequency[None, :]
    cosine = np.concatenate([np.cos(angle), np.cos(angle)], axis=1)
    sine = np.concatenate([-np.sin(angle), np.sin(angle)], axis=1)
    both = [np.concatenate([t, t], axis=0).astype(np.float32) for t in (cosine, sine)]
    return both


def attention_kernel(
    at_ref, same, other, gain, cos, sin, *refs
):
    weights, (keep_ref, send_ref, resid_ref) = refs[:4], refs[4:7]
    mixed_ref, (wq, wk, wv, wo), sems = refs[7], refs[8:12], refs[12]
    copies = [
        pltpu.make_async_copy(ref, to, sems.at[k])
        for k, (ref, to) in enumerate(zip(weights, (wq, wk, wv, wo)))
    ]
    for copy in copies:
        copy.start()
    x, c = at_ref[0], at_ref[1]
    m = x * 2 + c
    blocks = [same.at[t] for t in range(4)] + [other.at[t] for t in range(4)]

    def feature_block(k):
        return (k % 4) * 2 + (c if k < 4 else 1 - c)

    def piece(ref, col):
        return jnp.concatenate([ref[r * 4 + col] for r in range(8)], axis=0).astype(f32)

    squares = jnp.zeros((128, 128), f32)
    for ref in blocks:
        for col in range(4):
            v = piece(ref, col)
            squares = squares + v * v
    inv_rms = lax.rsqrt(jnp.sum(squares, axis=1, keepdims=True) * (1.0 / 4096.0) + norm_eps)

    for copy in copies[:3]:
        copy.wait()
    query = jnp.zeros((128, 256), f32)
    key = jnp.zeros((128, 128), f32)
    value = jnp.zeros((128, 128), f32)
    for k, ref in enumerate(blocks):
        fb = feature_block(k)
        g = gain[fb]
        normed = jnp.concatenate(
            [
                (piece(ref, col) * inv_rms * g[:, col * 128 : col * 128 + 128]).astype(bf16)
                for col in range(4)
            ],
            axis=1,
        )
        rows = pl.ds(pl.multiple_of(fb * 512, 512), 512)
        query = query + jnp.dot(normed, wq[rows, :], preferred_element_type=f32)
        key = key + jnp.dot(normed, wk[rows, :], preferred_element_type=f32)
        value = value + jnp.dot(normed, wv[rows, :], preferred_element_type=f32)

    def in_order(t):
        return jnp.concatenate(
            [t[r * 16 + s * 8 : r * 16 + s * 8 + 8] for s in range(2) for r in range(8)], axis=0
        )

    cosine, sine = cos[...], sin[...]

    def rotated(t):
        return (t * cosine + pltpu.roll(t, 64, axis=1) * sine).astype(bf16)

    query, key, value = in_order(query), rotated(in_order(key)), in_order(value).astype(bf16)
    row = lax.broadcasted_iota(i32, (128, 128), 0)
    column = lax.broadcasted_iota(i32, (128, 128), 1)
    seen = (row // SEQ_LEN == column // SEQ_LEN) & (column <= row)
    for h in range(2):
        q = rotated(query[:, h * 128 : h * 128 + 128])
        scores = lax.dot_general(q, key, (((1,), (1,)), ((), ())), preferred_element_type=f32)
        scores = jnp.where(seen, scores * HEAD_DIM ** (-0.5), -jnp.inf)
        top = jnp.max(scores, axis=1, keepdims=True)
        e = jnp.exp(scores - top)
        weights = (e / jnp.sum(e, axis=1, keepdims=True)).astype(bf16)
        mixed = jnp.dot(weights, value, preferred_element_type=f32).astype(bf16)
        mixed_ref[:, :, h * 128 : h * 128 + 128] = mixed.reshape(8, 16, 128)
    left = jnp.concatenate(
        [mixed_ref[t * 2 + c] for t in range(4)] + [mixed_ref[t * 2 + 1 - c] for t in range(4)],
        axis=0,
    )
    copies[3].wait()
    for fb in range(8):
        part = jnp.dot(left, wo[:, fb * 512 : fb * 512 + 512], preferred_element_type=f32)
        part = part.astype(bf16).reshape(8, 16, 512)
        keep_ref[:, fb] = part[:4]
        send_ref[:, fb] = part[4:]

    first = m < 4
    r0 = lax.rem(m, 4) * 2
    for k, ref in enumerate(blocks):
        fb = feature_block(k)
        rows = []
        for r in range(2):
            cols = []
            for col in range(4):
                v = ref[(r0 + r) * 4 + col].astype(f32)
                cols.append(jnp.where(first, v[:8], v[8:]))
            rows.append(jnp.concatenate(cols, axis=1))
        resid_ref[fb] = jnp.concatenate(rows, axis=0).astype(bf16)


def final_kernel(at_ref, resid, sums, gain, fa_ref, fb_ref, hidden_ref):
    x, c = at_ref[0], at_ref[1]
    squares = jnp.zeros((16, 512), f32)
    for k in range(8):
        h = resid[k].astype(f32) + (
            (sums[0, k].astype(f32) + sums[1, k].astype(f32))
            + (sums[2, k].astype(f32) + sums[3, k].astype(f32))
        )
        hidden_ref[k] = h
        squares = squares + h * h
    inv_rms = lax.rsqrt(jnp.sum(squares, axis=1, keepdims=True) * (1.0 / 4096.0) + norm_eps)
    for s in range(4):
        base = lax.rem(x + (4 - s), 4) * 2
        fa_ref[s] = (hidden_ref[base + c] * inv_rms * gain[base + c]).astype(bf16)
        other = base + 1 - c
        rows = (hidden_ref[other] * inv_rms * gain[other]).astype(bf16)
        for t in range(8):
            fb_ref[t, s] = rows


BLOCKS = 4
WIDTH = 512


FRONT = 256


def logits_kernel(at_ref, *refs):
    pieces, rows_a, rows_b, goal_ref = refs[:14], refs[14:22], refs[22:26], refs[26]
    (out_ref, buffer, rows_ref, logit_ref, top_ref, sum_ref, pick_ref, goals_ref,
     sems) = refs[27:]
    whole, starts, at = (0, 7), [], 0
    for p in range(14):
        starts.append(at)
        at += 512 if p in whole else 256

    def copies(j):
        column = pl.ds(pl.multiple_of(j * WIDTH, WIDTH), WIDTH)
        return [
            pltpu.make_async_copy(
                ref.at[:, column],
                buffer.at[j, pl.ds(starts[p], 512 if p in whole else 256)],
                sems.at[j, p],
            )
            for p, ref in enumerate(pieces)
        ]

    @pl.loop(0, BLOCKS)
    def _(j):
        for copy in copies(j):
            copy.start()

    eye = lax.broadcasted_iota(i32, (128, 128), 0) == lax.broadcasted_iota(i32, (128, 128), 1)
    for q in range(4):
        goals_ref[q * 128 : q * 128 + 128] = jnp.sum(
            jnp.where(eye, goal_ref[q : q + 1], 0.0), axis=1, keepdims=True
        )
    top_ref[...] = jnp.full((512, 1), -jnp.inf, f32)
    sum_ref[...] = jnp.zeros((512, 1), f32)
    pick_ref[...] = jnp.zeros((512, 1), f32)

    z, y = at_ref[2], at_ref[3]
    for dz in range(8):
        for dy in range(4):
            in_y = lax.rem(y + (4 - dy), 4)
            a_rows = pl.ds(pl.multiple_of((lax.rem(z + (8 - dz), 8) * 4 + in_y) * 16, 16), 16)
            b_rows = pl.ds(pl.multiple_of((dz * 4 + in_y) * 16, 16), 16)
            for k in range(4):
                rows_ref[a_rows, k * 512 : k * 512 + 512] = rows_a[dz][dy, k]
                rows_ref[b_rows, 2048 + k * 512 : 2560 + k * 512] = rows_b[dy][dz, k]

    def multiply(j):
        for copy in copies(j):
            copy.wait()
        return jnp.dot(rows_ref[...], buffer[j], preferred_element_type=f32)

    def reduce(j, logits):
        column = lax.broadcasted_iota(i32, logits.shape, 1).astype(f32)
        top = top_ref[...]
        new = jnp.maximum(top, jnp.max(logits, axis=1, keepdims=True))
        sum_ref[...] = sum_ref[...] * jnp.exp(top - new) + jnp.sum(
            jnp.exp(logits - new), axis=1, keepdims=True
        )
        hit = column == goals_ref[...] - lax.convert_element_type(j * WIDTH, f32)
        pick_ref[...] += jnp.sum(jnp.where(hit, logits, 0.0), axis=1, keepdims=True)
        top_ref[...] = new

    logit_ref[0] = multiply(0)

    @pl.loop(1, BLOCKS)
    def _(j):
        logits = multiply(j)
        reduce(j - 1, logit_ref[lax.rem(j - 1, 2)])
        logit_ref[lax.rem(j, 2)] = logits

    reduce(jnp.int32(BLOCKS - 1), logit_ref[(BLOCKS - 1) % 2])
    lines = []
    for values in (top_ref[...] + jnp.log(sum_ref[...]), pick_ref[...]):
        for q in range(4):
            block = jnp.where(eye, values[q * 128 : q * 128 + 128], 0.0)
            lines.append(jnp.sum(block, axis=0, keepdims=True))
    lines = jnp.concatenate(lines, axis=0)
    for t in range(32):
        out_ref[t] = lines


def logits_call(at, weights, rows, goals):
    vmem = pl.BlockSpec(memory_space=pltpu.VMEM)
    hbm = pl.BlockSpec(memory_space=pltpu.HBM)
    return pl.pallas_call(
        logits_kernel,
        out_shape=sds((32, 8, 128), f32),
        in_specs=[pl.BlockSpec(memory_space=pltpu.SMEM)]
        + [hbm] * len(weights)
        + [vmem] * (len(rows) + 1),
        out_specs=vmem,
        scratch_shapes=[
            pltpu.VMEM((BLOCKS, 4096, WIDTH), bf16),
            pltpu.VMEM((512, 4096), bf16),
            pltpu.VMEM((2, 512, WIDTH), f32),
            pltpu.VMEM((512, 1), f32),
            pltpu.VMEM((512, 1), f32),
            pltpu.VMEM((512, 1), f32),
            pltpu.VMEM((512, 1), f32),
            pltpu.SemaphoreType.DMA((BLOCKS, 14)),
        ],
        name="logits",
        cost_estimate=pl.CostEstimate(
            flops=2 * 512 * 4096 * 2048, bytes_accessed=20 << 20, transcendentals=0
        ),
        compiler_params=pltpu.CompilerParams(vmem_limit_bytes=36 << 20),
    )(at, *weights, *rows, goals)


def merge_kernel(got_ref, label_ref, loss_ref, sums_ref):
    lse = [got_ref[k][:4] for k in range(32)]
    top = functools.reduce(jnp.maximum, lse)
    total = functools.reduce(lambda a, b: a + b, [jnp.exp(v - top) for v in lse])
    picked = functools.reduce(lambda a, b: a + b, [got_ref[k][4:] for k in range(32)])
    loss = top + jnp.log(total) - picked
    loss_ref[...] = loss
    domain = lax.broadcasted_iota(i32, (128, 128), 0)
    by_domain = jnp.zeros((128, 128), f32)
    for q in range(4):
        same = domain == label_ref[q : q + 1, :]
        by_domain = by_domain + jnp.where(same, loss[q : q + 1, :], 0.0)
    column = jnp.sum(by_domain, axis=1, keepdims=True)
    eye = domain == lax.broadcasted_iota(i32, (128, 128), 1)
    line = jnp.sum(jnp.where(eye, column, 0.0), axis=0, keepdims=True)
    for t in range(8):
        sums_ref[t] = jnp.broadcast_to(line, (8, 128))


def output_kernel(sums_ref, tally, prev, old, new_ref, probs_ref):
    sums = sums_ref[0]
    for t in range(1, 8):
        sums = sums + sums_ref[t]
    sums = sums[0:1]
    reward = sums / jnp.maximum(tally[...], 1.0) / prev[...]
    new = memory_rate * old[...] + (1.0 - memory_rate) * reward
    real = lax.broadcasted_iota(i32, (1, 128), 1) < DOMAINS
    scaled = jnp.where(real, step_rate * new, -jnp.inf)
    e = jnp.exp(scaled - jnp.max(scaled, axis=1, keepdims=True))
    soft = e / jnp.sum(e, axis=1, keepdims=True)
    new_ref[...] = new[:, :DOMAINS]
    probs_ref[...] = ((1.0 - DOMAINS * explore_mass) * soft + explore_mass)[:, :DOMAINS]


def program(
    embedded, targets, labels, counts, destinations, gain_in, w_query, w_key, w_value, w_out,
    gain_out, w_vocab, prev_probs, log_weights,
):
    z, y, x, c = (lax.axis_index(a) for a in ALL)
    d, m = z * NY + y, x * NC + c
    at = jnp.stack([x, c, z, y]).astype(i32)

    w_other = shift(w_vocab, "c", 1)
    rows = w_vocab[:FRONT]
    front_1, front_3 = shift(rows, "x", 1), shift(rows, "x", 3)

    packed = call(
        pack_kernel, sds((32, 5, 8, 128), bf16),
        (embedded, targets, labels.reshape(1, 4), destinations.reshape(1, 4)),
        scratch=[pltpu.VMEM((8, 128), f32)], vmem=60,
    )
    got = lax.all_to_all(packed, DP, 0, 0, tiled=True)

    meta = got[:, 4]
    label_of = meta[:, 4, 0:4].reshape(128).astype(i32)
    goes_to = meta[:, 5, 0:4].reshape(128).astype(i32)
    slot = jnp.arange(128, dtype=i32)
    live = slot % 4 < jnp.repeat(counts, 4)
    chosen = live[None, :] & (goes_to[None, :] == jnp.arange(64, dtype=i32)[:, None])
    source_row = jnp.sum(jnp.where(chosen, (slot // 4) * 5 + slot % 4, 0), axis=1)
    picked = call(select_kernel, sds((64, 8, 128), bf16), (got.reshape(160, 8, 128),), source_row)
    block = lax.all_to_all(picked.reshape(32, 16, 128), DP, 0, 0, tiled=True)

    same = lax.all_gather(block, "x", axis=0, tiled=False)
    other = shift(same, "c", 1)

    cosine, sine = rope_tables()
    keep, send, resid = call(
        attention_kernel,
        [sds((4, 8, 16, 512), bf16), sds((4, 8, 16, 512), bf16), sds((8, 16, 512), bf16)],
        (
            same, other, gain_in.reshape(8, 1, 512), jnp.asarray(cosine), jnp.asarray(sine),
            w_query, w_key, w_value, w_out,
        ),
        at,
        scratch=[pltpu.VMEM((8, 16, 256), bf16)]
        + [pltpu.VMEM(w.shape, bf16) for w in (w_query, w_key, w_value, w_out)]
        + [pltpu.SemaphoreType.DMA((4,))],
        flops=1 << 30,
        vmem=48,
        far=4,
    )
    got_part = shift(send, "c", 1)
    pair = (keep.astype(f32) + got_part.astype(f32)).astype(bf16)
    sums = lax.all_to_all(pair, "x", 0, 0, tiled=True)

    rows = w_vocab[FRONT:]
    late_1, late_3 = shift(rows, "x", 1), shift(rows, "x", 3)
    front_2 = shift(front_1, "x", 1)
    late_2 = shift(late_3, "x", 3)
    core_front_1, core_front_3 = shift(front_1, "c", 1), shift(front_3, "c", 1)
    core_late_1, core_late_3 = shift(late_1, "c", 1), shift(late_3, "c", 1)
    core_front_2, core_late_2 = shift(front_2, "c", 1), shift(late_2, "c", 1)

    seq_ids = jnp.dot(
        chosen.astype(bf16), meta[:, :4].reshape(128, 128), preferred_element_type=f32
    ).astype(i32)
    seq_goals = seq_ids[:, :64] * 256 + seq_ids[:, 64:]
    seq_labels = jnp.sum(jnp.where(chosen, label_of[None, :], 0), axis=1)
    mine = lax.dynamic_slice(
        seq_goals.reshape(32, 2, 4, 16), (0, m // 4, m % 4, 0), (32, 1, 1, 16)
    ).reshape(512)
    kinds = lax.dynamic_slice(seq_labels.reshape(32, 2), (0, m // 4), (32, 1))
    kinds = jnp.broadcast_to(kinds, (32, 16)).reshape(4, 128)
    goals = (mine - d * 2048).astype(f32).reshape(4, 128)
    domain = jnp.arange(128, dtype=i32)
    tally = SEQ_LEN * jnp.sum(
        (live[:, None] & (label_of[:, None] == domain[None, :])).astype(f32), axis=0
    )
    sums, goals = lax.optimization_barrier((sums, goals))

    fa, fb = call(
        final_kernel, [sds((4, 16, 512), bf16), sds((8, 4, 16, 512), bf16)],
        (resid, sums, gain_out.reshape(8, 1, 512)), at,
        scratch=[pltpu.VMEM((8, 16, 512), f32)],
    )

    parts = [shift(fa, "y", s) for s in (1, 2, 3)]
    column = lax.all_to_all(fb, "z", 0, 0, tiled=True)
    group = jnp.stack([fa, *parts])
    up, down = [group], [group]
    for _ in range(3):
        up.append(shift(up[-1], "z", 1))
        down.append(shift(down[-1], "z", NZ - 1))
    rows_b = [column] + [shift(column, "y", s) for s in (1, 2, 3)]
    up.append(shift(up[-1], "z", 1))
    rows_a = [*up, down[3], down[2], down[1]]
    weights = (
        w_vocab, front_1, late_1, front_2, late_2, front_3, late_3,
        w_other, core_front_1, core_late_1, core_front_2, core_late_2, core_front_3, core_late_3,
    )
    pieces = logits_call(at, weights, (*rows_a, *rows_b), goals)
    merged = lax.all_to_all(pieces, DP, 0, 0, tiled=True)
    losses, sums_here = call(
        merge_kernel, [sds((4, 128), f32), sds((8, 8, 128), f32)], (merged, kinds)
    )
    own_loss = lax.dynamic_slice_in_dim(losses.reshape(512), d * 16, 16, 0)
    all_sums = lax.all_to_all(sums_here, MP, 0, 0, tiled=True)
    line = lambda v, fill: jnp.pad(v, (0, 128 - DOMAINS), constant_values=fill).reshape(1, 128)
    new_weights, probs = call(
        output_kernel, [sds((1, DOMAINS), f32)] * 2,
        (all_sums, tally.reshape(1, 128), line(prev_probs, 1.0), line(log_weights, 0.0)),
    )
    return own_loss, new_weights.reshape(DOMAINS), probs.reshape(DOMAINS)


def solution(mesh):
    torus = Mesh(mesh.devices.reshape(NZ, NY, NX, NC), ALL)
    in_specs = (
        P(DP, None, MP), P(DP, None), P(DP), P(), P(DP), P(), P(None, MP), P(None, MP),
        P(None, MP), P(MP, None), P(), P(MP, DP), P(), P(),
    )
    return jax.shard_map(
        program, mesh=torus, in_specs=in_specs, out_specs=(P(ALL), P(), P()), check_vma=False
    )
```

```python
import functools

import jax
import jax.numpy as jnp
import numpy as np
from jax import lax
from jax.experimental import pallas as pl
from jax.experimental.pallas import tpu as pltpu
from jax.sharding import Mesh
from jax.sharding import PartitionSpec as P


HEAD_DIM = 128
DOMAINS = 22
SEQ_LEN = 64
DP = ("z", "y")
MP = ("x", "c")
ALL = ("z", "y", "x", "c")
NZ, NY, NX, NC = 8, 4, 4, 2

norm_eps = 1e-05
rope_base = 500000.0
memory_rate = 0.9
step_rate = 0.02
explore_mass = 0.005


bf16 = jnp.bfloat16
f32 = jnp.float32
i32 = jnp.int32


def shift(array, axis, by):
    n = {"z": NZ, "y": NY, "x": NX, "c": NC}[axis]
    return lax.ppermute(array, axis, [(i, (i + by) % n) for i in range(n)])


def call(kernel, out_shape, args, scalars=None, scratch=(), flops=0, vmem=4, far=0):
    spec = pl.BlockSpec(memory_space=pltpu.VMEM)
    many = isinstance(out_shape, (list, tuple))
    return pl.pallas_call(
        kernel,
        out_shape=out_shape,
        in_specs=([pl.BlockSpec(memory_space=pltpu.SMEM)] if scalars is not None else [])
        + [spec] * (len(args) - far)
        + [pl.BlockSpec(memory_space=pltpu.HBM)] * far,
        out_specs=[spec] * len(out_shape) if many else spec,
        scratch_shapes=scratch,
        compiler_params=pltpu.CompilerParams(vmem_limit_bytes=vmem << 20),
        cost_estimate=pl.CostEstimate(flops=flops, bytes_accessed=0, transcendentals=0)
        if flops
        else None,
    )(*(() if scalars is None else (scalars,)), *args)


def sds(shape, dtype):
    return jax.ShapeDtypeStruct(shape, dtype)


def pack_kernel(embedded, targets, labels, destinations, out_ref, meta_ref):
    ids = targets[...]
    meta_ref[...] = jnp.zeros((8, 128), f32)
    meta_ref[0:4, 0:64] = (ids // 256).astype(f32)
    meta_ref[0:4, 64:128] = (ids % 256).astype(f32)
    meta_ref[4:5, 0:4] = labels[...].astype(f32)
    meta_ref[5:6, 0:4] = destinations[...].astype(f32)
    meta = meta_ref[...].astype(bf16)
    for r in range(8):
        for col in range(4):
            for s in range(4):
                out_ref[r * 4 + col, s] = embedded[
                    s, r * 8 : r * 8 + 8, col * 128 : col * 128 + 128
                ]
            out_ref[r * 4 + col, 4] = meta


def select_kernel(row_ref, got_ref, out_ref):
    for g in range(64):
        out_ref[g] = got_ref[row_ref[g]]


def rope_tables():
    half = HEAD_DIM // 2
    frequency = np.power(rope_base, -np.arange(half) * 2.0 / HEAD_DIM)
    angle = np.arange(SEQ_LEN)[:, None] * frequency[None, :]
    cosine = np.concatenate([np.cos(angle), np.cos(angle)], axis=1)
    sine = np.concatenate([-np.sin(angle), np.sin(angle)], axis=1)
    both = [np.concatenate([t, t], axis=0).astype(np.float32) for t in (cosine, sine)]
    return both


def attention_kernel(
    at_ref, same, other, gain, cos, sin, *refs
):
    weights, (keep_ref, send_ref, resid_ref) = refs[:4], refs[4:7]
    mixed_ref, (wq, wk, wv, wo), sems = refs[7], refs[8:12], refs[12]
    copies = [
        pltpu.make_async_copy(ref, to, sems.at[k])
        for k, (ref, to) in enumerate(zip(weights, (wq, wk, wv, wo)))
    ]
    for copy in copies:
        copy.start()
    x, c = at_ref[0], at_ref[1]
    m = x * 2 + c
    blocks = [same.at[t] for t in range(4)] + [other.at[t] for t in range(4)]

    def feature_block(k):
        return (k % 4) * 2 + (c if k < 4 else 1 - c)

    def piece(ref, col):
        return jnp.concatenate([ref[r * 4 + col] for r in range(8)], axis=0).astype(f32)

    squares = jnp.zeros((128, 128), f32)
    for ref in blocks:
        for col in range(4):
            v = piece(ref, col)
            squares = squares + v * v
    inv_rms = lax.rsqrt(jnp.sum(squares, axis=1, keepdims=True) * (1.0 / 4096.0) + norm_eps)

    for copy in copies[:3]:
        copy.wait()
    query = jnp.zeros((128, 256), f32)
    key = jnp.zeros((128, 128), f32)
    value = jnp.zeros((128, 128), f32)
    for k, ref in enumerate(blocks):
        fb = feature_block(k)
        g = gain[fb]
        normed = jnp.concatenate(
            [
                (piece(ref, col) * inv_rms * g[:, col * 128 : col * 128 + 128]).astype(bf16)
                for col in range(4)
            ],
            axis=1,
        )
        rows = pl.ds(pl.multiple_of(fb * 512, 512), 512)
        query = query + jnp.dot(normed, wq[rows, :], preferred_element_type=f32)
        key = key + jnp.dot(normed, wk[rows, :], preferred_element_type=f32)
        value = value + jnp.dot(normed, wv[rows, :], preferred_element_type=f32)

    def in_order(t):
        return jnp.concatenate(
            [t[r * 16 + s * 8 : r * 16 + s * 8 + 8] for s in range(2) for r in range(8)], axis=0
        )

    cosine, sine = cos[...], sin[...]

    def rotated(t):
        return (t * cosine + pltpu.roll(t, 64, axis=1) * sine).astype(bf16)

    query, key, value = in_order(query), rotated(in_order(key)), in_order(value).astype(bf16)
    row = lax.broadcasted_iota(i32, (128, 128), 0)
    column = lax.broadcasted_iota(i32, (128, 128), 1)
    seen = (row // SEQ_LEN == column // SEQ_LEN) & (column <= row)
    for h in range(2):
        q = rotated(query[:, h * 128 : h * 128 + 128])
        scores = lax.dot_general(q, key, (((1,), (1,)), ((), ())), preferred_element_type=f32)
        scores = jnp.where(seen, scores * HEAD_DIM ** (-0.5), -jnp.inf)
        top = jnp.max(scores, axis=1, keepdims=True)
        e = jnp.exp(scores - top)
        weights = (e / jnp.sum(e, axis=1, keepdims=True)).astype(bf16)
        mixed = jnp.dot(weights, value, preferred_element_type=f32).astype(bf16)
        mixed_ref[:, :, h * 128 : h * 128 + 128] = mixed.reshape(8, 16, 128)
    left = jnp.concatenate(
        [mixed_ref[t * 2 + c] for t in range(4)] + [mixed_ref[t * 2 + 1 - c] for t in range(4)],
        axis=0,
    )
    copies[3].wait()
    for fb in range(8):
        part = jnp.dot(left, wo[:, fb * 512 : fb * 512 + 512], preferred_element_type=f32)
        part = part.astype(bf16).reshape(8, 16, 512)
        keep_ref[:, fb] = part[:4]
        send_ref[:, fb] = part[4:]

    first = m < 4
    r0 = lax.rem(m, 4) * 2
    for k, ref in enumerate(blocks):
        fb = feature_block(k)
        rows = []
        for r in range(2):
            cols = []
            for col in range(4):
                v = ref[(r0 + r) * 4 + col].astype(f32)
                cols.append(jnp.where(first, v[:8], v[8:]))
            rows.append(jnp.concatenate(cols, axis=1))
        resid_ref[fb] = jnp.concatenate(rows, axis=0).astype(bf16)


def final_kernel(at_ref, resid, sums, gain, fa_ref, fb_ref, hidden_ref):
    x, c = at_ref[0], at_ref[1]
    squares = jnp.zeros((16, 512), f32)
    for k in range(8):
        h = resid[k].astype(f32) + (
            (sums[0, k].astype(f32) + sums[1, k].astype(f32))
            + (sums[2, k].astype(f32) + sums[3, k].astype(f32))
        )
        hidden_ref[k] = h
        squares = squares + h * h
    inv_rms = lax.rsqrt(jnp.sum(squares, axis=1, keepdims=True) * (1.0 / 4096.0) + norm_eps)
    for s in range(4):
        base = lax.rem(x + (4 - s), 4) * 2
        fa_ref[s] = (hidden_ref[base + c] * inv_rms * gain[base + c]).astype(bf16)
        other = base + 1 - c
        rows = (hidden_ref[other] * inv_rms * gain[other]).astype(bf16)
        for t in range(8):
            fb_ref[t, s] = rows


BLOCKS = 4
WIDTH = 512


FRONT = 256


def logits_kernel(at_ref, *refs):
    pieces, rows_a, rows_b, goal_ref = refs[:14], refs[14:22], refs[22:26], refs[26]
    (out_ref, buffer, rows_ref, logit_ref, top_ref, sum_ref, pick_ref, goals_ref,
     sems) = refs[27:]
    whole, starts, at = (0, 7), [], 0
    for p in range(14):
        starts.append(at)
        at += 512 if p in whole else 256

    def copies(j):
        column = pl.ds(pl.multiple_of(j * WIDTH, WIDTH), WIDTH)
        return [
            pltpu.make_async_copy(
                ref.at[:, column],
                buffer.at[j, pl.ds(starts[p], 512 if p in whole else 256)],
                sems.at[j, p],
            )
            for p, ref in enumerate(pieces)
        ]

    for copy in copies(0):
        copy.start()

    eye = lax.broadcasted_iota(i32, (128, 128), 0) == lax.broadcasted_iota(i32, (128, 128), 1)
    for q in range(4):
        goals_ref[q * 128 : q * 128 + 128] = jnp.sum(
            jnp.where(eye, goal_ref[q : q + 1], 0.0), axis=1, keepdims=True
        )
    top_ref[...] = jnp.full((512, 1), -jnp.inf, f32)
    sum_ref[...] = jnp.zeros((512, 1), f32)
    pick_ref[...] = jnp.zeros((512, 1), f32)

    z, y = at_ref[2], at_ref[3]
    for dz in range(8):
        for dy in range(4):
            in_y = lax.rem(y + (4 - dy), 4)
            a_rows = pl.ds(pl.multiple_of((lax.rem(z + (8 - dz), 8) * 4 + in_y) * 16, 16), 16)
            b_rows = pl.ds(pl.multiple_of((dz * 4 + in_y) * 16, 16), 16)
            for k in range(4):
                rows_ref[a_rows, k * 512 : k * 512 + 512] = rows_a[dz][dy, k]
                rows_ref[b_rows, 2048 + k * 512 : 2560 + k * 512] = rows_b[dy][dz, k]

    for copy in copies(1):
        copy.start()

    def multiply(j):
        for copy in copies(j):
            copy.wait()
        return jnp.dot(rows_ref[...], buffer[j], preferred_element_type=f32)

    def reduce(j, logits):
        column = lax.broadcasted_iota(i32, logits.shape, 1).astype(f32)
        top = top_ref[...]
        new = jnp.maximum(top, jnp.max(logits, axis=1, keepdims=True))
        sum_ref[...] = sum_ref[...] * jnp.exp(top - new) + jnp.sum(
            jnp.exp(logits - new), axis=1, keepdims=True
        )
        hit = column == goals_ref[...] - lax.convert_element_type(j * WIDTH, f32)
        pick_ref[...] += jnp.sum(jnp.where(hit, logits, 0.0), axis=1, keepdims=True)
        top_ref[...] = new

    logit_ref[0] = multiply(0)

    @pl.loop(1, BLOCKS)
    def _(j):
        @pl.when(j + 1 < BLOCKS)
        def _():
            for copy in copies(j + 1):
                copy.start()

        logits = multiply(j)
        reduce(j - 1, logit_ref[lax.rem(j - 1, 2)])
        logit_ref[lax.rem(j, 2)] = logits

    reduce(jnp.int32(BLOCKS - 1), logit_ref[(BLOCKS - 1) % 2])
    lines = []
    for values in (top_ref[...] + jnp.log(sum_ref[...]), pick_ref[...]):
        for q in range(4):
            block = jnp.where(eye, values[q * 128 : q * 128 + 128], 0.0)
            lines.append(jnp.sum(block, axis=0, keepdims=True))
    lines = jnp.concatenate(lines, axis=0)
    for t in range(32):
        out_ref[t] = lines


def logits_call(at, weights, rows, goals):
    vmem = pl.BlockSpec(memory_space=pltpu.VMEM)
    hbm = pl.BlockSpec(memory_space=pltpu.HBM)
    return pl.pallas_call(
        logits_kernel,
        out_shape=sds((32, 8, 128), f32),
        in_specs=[pl.BlockSpec(memory_space=pltpu.SMEM)]
        + [hbm] * len(weights)
        + [vmem] * (len(rows) + 1),
        out_specs=vmem,
        scratch_shapes=[
            pltpu.VMEM((BLOCKS, 4096, WIDTH), bf16),
            pltpu.VMEM((512, 4096), bf16),
            pltpu.VMEM((2, 512, WIDTH), f32),
            pltpu.VMEM((512, 1), f32),
            pltpu.VMEM((512, 1), f32),
            pltpu.VMEM((512, 1), f32),
            pltpu.VMEM((512, 1), f32),
            pltpu.SemaphoreType.DMA((BLOCKS, 14)),
        ],
        name="logits",
        cost_estimate=pl.CostEstimate(
            flops=2 * 512 * 4096 * 2048, bytes_accessed=20 << 20, transcendentals=0
        ),
        compiler_params=pltpu.CompilerParams(vmem_limit_bytes=36 << 20),
    )(at, *weights, *rows, goals)


def merge_kernel(got_ref, label_ref, loss_ref, sums_ref):
    lse = [got_ref[k][:4] for k in range(32)]
    top = functools.reduce(jnp.maximum, lse)
    total = functools.reduce(lambda a, b: a + b, [jnp.exp(v - top) for v in lse])
    picked = functools.reduce(lambda a, b: a + b, [got_ref[k][4:] for k in range(32)])
    loss = top + jnp.log(total) - picked
    loss_ref[...] = loss
    domain = lax.broadcasted_iota(i32, (128, 128), 0)
    by_domain = jnp.zeros((128, 128), f32)
    for q in range(4):
        same = domain == label_ref[q : q + 1, :]
        by_domain = by_domain + jnp.where(same, loss[q : q + 1, :], 0.0)
    column = jnp.sum(by_domain, axis=1, keepdims=True)
    eye = domain == lax.broadcasted_iota(i32, (128, 128), 1)
    line = jnp.sum(jnp.where(eye, column, 0.0), axis=0, keepdims=True)
    for t in range(8):
        sums_ref[t] = jnp.broadcast_to(line, (8, 128))


def output_kernel(sums_ref, tally, prev, old, new_ref, probs_ref):
    sums = sums_ref[0]
    for t in range(1, 8):
        sums = sums + sums_ref[t]
    sums = sums[0:1]
    reward = sums / jnp.maximum(tally[...], 1.0) / prev[...]
    new = memory_rate * old[...] + (1.0 - memory_rate) * reward
    real = lax.broadcasted_iota(i32, (1, 128), 1) < DOMAINS
    scaled = jnp.where(real, step_rate * new, -jnp.inf)
    e = jnp.exp(scaled - jnp.max(scaled, axis=1, keepdims=True))
    soft = e / jnp.sum(e, axis=1, keepdims=True)
    new_ref[...] = new[:, :DOMAINS]
    probs_ref[...] = ((1.0 - DOMAINS * explore_mass) * soft + explore_mass)[:, :DOMAINS]


def program(
    embedded, targets, labels, counts, destinations, gain_in, w_query, w_key, w_value, w_out,
    gain_out, w_vocab, prev_probs, log_weights,
):
    z, y, x, c = (lax.axis_index(a) for a in ALL)
    d, m = z * NY + y, x * NC + c
    at = jnp.stack([x, c, z, y]).astype(i32)

    w_other = shift(w_vocab, "c", 1)
    rows = w_vocab[:FRONT]
    front_1, front_3 = shift(rows, "x", 1), shift(rows, "x", 3)

    packed = call(
        pack_kernel, sds((32, 5, 8, 128), bf16),
        (embedded, targets, labels.reshape(1, 4), destinations.reshape(1, 4)),
        scratch=[pltpu.VMEM((8, 128), f32)], vmem=60,
    )
    got = lax.all_to_all(packed, DP, 0, 0, tiled=True)

    meta = got[:, 4]
    label_of = meta[:, 4, 0:4].reshape(128).astype(i32)
    goes_to = meta[:, 5, 0:4].reshape(128).astype(i32)
    slot = jnp.arange(128, dtype=i32)
    live = slot % 4 < jnp.repeat(counts, 4)
    chosen = live[None, :] & (goes_to[None, :] == jnp.arange(64, dtype=i32)[:, None])
    source_row = jnp.sum(jnp.where(chosen, (slot // 4) * 5 + slot % 4, 0), axis=1)
    picked = call(select_kernel, sds((64, 8, 128), bf16), (got.reshape(160, 8, 128),), source_row)
    block = lax.all_to_all(picked.reshape(32, 16, 128), DP, 0, 0, tiled=True)

    same = lax.all_gather(block, "x", axis=0, tiled=False)
    other = shift(same, "c", 1)

    cosine, sine = rope_tables()
    keep, send, resid = call(
        attention_kernel,
        [sds((4, 8, 16, 512), bf16), sds((4, 8, 16, 512), bf16), sds((8, 16, 512), bf16)],
        (
            same, other, gain_in.reshape(8, 1, 512), jnp.asarray(cosine), jnp.asarray(sine),
            w_query, w_key, w_value, w_out,
        ),
        at,
        scratch=[pltpu.VMEM((8, 16, 256), bf16)]
        + [pltpu.VMEM(w.shape, bf16) for w in (w_query, w_key, w_value, w_out)]
        + [pltpu.SemaphoreType.DMA((4,))],
        flops=1 << 30,
        vmem=48,
        far=4,
    )
    got_part = shift(send, "c", 1)
    pair = (keep.astype(f32) + got_part.astype(f32)).astype(bf16)
    sums = lax.all_to_all(pair, "x", 0, 0, tiled=True)

    rows = w_vocab[FRONT:]
    late_1, late_3 = shift(rows, "x", 1), shift(rows, "x", 3)
    front_2 = shift(front_1, "x", 1)
    late_2 = shift(late_3, "x", 3)
    core_front_1, core_front_3 = shift(front_1, "c", 1), shift(front_3, "c", 1)
    core_late_1, core_late_3 = shift(late_1, "c", 1), shift(late_3, "c", 1)
    core_front_2, core_late_2 = shift(front_2, "c", 1), shift(late_2, "c", 1)

    seq_ids = jnp.dot(
        chosen.astype(bf16), meta[:, :4].reshape(128, 128), preferred_element_type=f32
    ).astype(i32)
    seq_goals = seq_ids[:, :64] * 256 + seq_ids[:, 64:]
    seq_labels = jnp.sum(jnp.where(chosen, label_of[None, :], 0), axis=1)
    mine = lax.dynamic_slice(
        seq_goals.reshape(32, 2, 4, 16), (0, m // 4, m % 4, 0), (32, 1, 1, 16)
    ).reshape(512)
    kinds = lax.dynamic_slice(seq_labels.reshape(32, 2), (0, m // 4), (32, 1))
    kinds = jnp.broadcast_to(kinds, (32, 16)).reshape(4, 128)
    goals = (mine - d * 2048).astype(f32).reshape(4, 128)
    domain = jnp.arange(128, dtype=i32)
    tally = SEQ_LEN * jnp.sum(
        (live[:, None] & (label_of[:, None] == domain[None, :])).astype(f32), axis=0
    )
    sums, goals = lax.optimization_barrier((sums, goals))

    fa, fb = call(
        final_kernel, [sds((4, 16, 512), bf16), sds((8, 4, 16, 512), bf16)],
        (resid, sums, gain_out.reshape(8, 1, 512)), at,
        scratch=[pltpu.VMEM((8, 16, 512), f32)],
    )

    parts = [shift(fa, "y", s) for s in (1, 2, 3)]
    column = lax.all_to_all(fb, "z", 0, 0, tiled=True)
    group = jnp.stack([fa, *parts])
    up, down = [group], [group]
    for _ in range(3):
        up.append(shift(up[-1], "z", 1))
        down.append(shift(down[-1], "z", NZ - 1))
    rows_b = [column] + [shift(column, "y", s) for s in (1, 2, 3)]
    up.append(shift(up[-1], "z", 1))
    rows_a = [*up, down[3], down[2], down[1]]
    weights = (
        w_vocab, front_1, late_1, front_2, late_2, front_3, late_3,
        w_other, core_front_1, core_late_1, core_front_2, core_late_2, core_front_3, core_late_3,
    )
    pieces = logits_call(at, weights, (*rows_a, *rows_b), goals)
    merged = lax.all_to_all(pieces, DP, 0, 0, tiled=True)
    losses, sums_here = call(
        merge_kernel, [sds((4, 128), f32), sds((8, 8, 128), f32)], (merged, kinds)
    )
    own_loss = lax.dynamic_slice_in_dim(losses.reshape(512), d * 16, 16, 0)
    all_sums = lax.all_to_all(sums_here, MP, 0, 0, tiled=True)
    line = lambda v, fill: jnp.pad(v, (0, 128 - DOMAINS), constant_values=fill).reshape(1, 128)
    new_weights, probs = call(
        output_kernel, [sds((1, DOMAINS), f32)] * 2,
        (all_sums, tally.reshape(1, 128), line(prev_probs, 1.0), line(log_weights, 0.0)),
    )
    return own_loss, new_weights.reshape(DOMAINS), probs.reshape(DOMAINS)


def solution(mesh):
    torus = Mesh(mesh.devices.reshape(NZ, NY, NX, NC), ALL)
    in_specs = (
        P(DP, None, MP), P(DP, None), P(DP), P(), P(DP), P(), P(None, MP), P(None, MP),
        P(None, MP), P(MP, None), P(), P(MP, DP), P(), P(),
    )
    return jax.shard_map(
        program, mesh=torus, in_specs=in_specs, out_specs=(P(ALL), P(), P()), check_vma=False
    )
```
